128 devices in a mesh: dp: 1, tp: 16 (over z, y), fsdp: 8 (over x, core).
Axes of the slice: x: 4, y: 4, z: 4, core: 2. Of those that a mesh axis runs over, the one named last changes fastest.
Arguments:
- hidden: bfloat16 [8, 1024, 6144], P(('dp', 'fsdp'))
- positions: int32 [1024], replicated
- norm_gain: float32 [6144], P('fsdp')
- w_query: bfloat16 [6144, 6144], P('fsdp', 'tp')
- w_key: bfloat16 [6144, 96], P('fsdp')
- w_value: bfloat16 [6144, 96], P('fsdp')
- w_gate: bfloat16 [6144, 24576], P('fsdp', 'tp')
- w_up: bfloat16 [6144, 24576], P('fsdp', 'tp')
- w_out: bfloat16 [6144, 6144], P('tp', 'fsdp')
- w_down: bfloat16 [24576, 6144], P('tp', 'fsdp')
Outputs:
- output: bfloat16 [8, 1024, 6144], P(('dp', 'fsdp'))
All inputs are finite; a program needn't handle non-finite values.
Results may differ from the reference program's by a relative error of at most 0.0118586.
Values are sent between devices in bfloat16 or wider.
A program may use at most 1 GiB of HBM per device.

```python
import jax
import jax.numpy as jnp
from jax import lax

BATCH_ROWS = 8
SEQ_LEN = 1024
D_MODEL = 6144
N_HEADS = 64
HEAD_DIM = 96
D_FF = 24576


def setup_inputs(seed: int = 0, part: int = 0) -> dict:
    key_list = jax.random.split(jax.random.key(seed), 11)
    row_key = jax.random.fold_in(key_list[0], part)
    d_scale = D_MODEL ** -0.5
    q_width = N_HEADS * HEAD_DIM
    hidden = jax.random.normal(row_key, (BATCH_ROWS, SEQ_LEN, D_MODEL), jnp.float32)
    pos_steps = jax.random.randint(key_list[1], (SEQ_LEN,), 1, 3, dtype=jnp.int32)
    offset = jax.random.randint(key_list[2], (), 0, 1024, dtype=jnp.int32)
    positions = (offset + jnp.cumsum(pos_steps) - pos_steps[0]).astype(jnp.int32)
    norm_gain = jax.random.uniform(key_list[3], (D_MODEL,), jnp.float32, 0.5, 1.5)
    w_query = 2.0 * d_scale * jax.random.normal(key_list[4], (D_MODEL, q_width), jnp.float32)
    w_key = d_scale * jax.random.normal(key_list[5], (D_MODEL, HEAD_DIM), jnp.float32)
    w_value = d_scale * jax.random.normal(key_list[6], (D_MODEL, HEAD_DIM), jnp.float32)
    w_gate = d_scale * jax.random.normal(key_list[7], (D_MODEL, D_FF), jnp.float32)
    w_up = d_scale * jax.random.normal(key_list[8], (D_MODEL, D_FF), jnp.float32)
    w_out = q_width ** -0.5 * jax.random.normal(key_list[9], (q_width, D_MODEL), jnp.float32)
    w_down = D_FF ** -0.5 * jax.random.normal(key_list[10], (D_FF, D_MODEL), jnp.float32)
    return {
        "hidden": hidden.astype(jnp.bfloat16),
        "positions": positions,
        "norm_gain": norm_gain,
        "w_query": w_query.astype(jnp.bfloat16),
        "w_key": w_key.astype(jnp.bfloat16),
        "w_value": w_value.astype(jnp.bfloat16),
        "w_gate": w_gate.astype(jnp.bfloat16),
        "w_up": w_up.astype(jnp.bfloat16),
        "w_out": w_out.astype(jnp.bfloat16),
        "w_down": w_down.astype(jnp.bfloat16),
    }


def rope_tables(positions, head_dim):
    inv_freq = 10000.0 ** (-jnp.arange(0, head_dim, 2, dtype=jnp.float32) / head_dim)
    angles = positions.astype(jnp.float32)[:, None] * inv_freq[None, :]
    angles = jnp.concatenate([angles, angles], axis=-1)
    return jnp.cos(angles), jnp.sin(angles)


def rope_rotate(vectors, cos_t, sin_t):
    half_dim = vectors.shape[-1] // 2
    rotated = jnp.concatenate([-vectors[..., half_dim:], vectors[..., :half_dim]], axis=-1)
    return vectors * cos_t + rotated * sin_t


def layer_norm(hidden, gain_vec):
    row_f32 = hidden.astype(jnp.float32)
    centered = row_f32 - jnp.mean(row_f32, axis=-1, keepdims=True)
    variance = jnp.mean(centered * centered, axis=-1, keepdims=True)
    return (centered * lax.rsqrt(variance + 1e-6) * gain_vec).astype(jnp.bfloat16)


def reference(hidden, positions, norm_gain, w_query, w_key, w_value, w_gate, w_up, w_out, w_down):
    cos_t, sin_t = rope_tables(positions, HEAD_DIM)
    q_block = min(256, SEQ_LEN)
    n_blocks = SEQ_LEN // q_block
    score_scale = HEAD_DIM ** -0.5
    key_index = jnp.arange(SEQ_LEN)

    def seq_layer(seq_rows):
        normed = layer_norm(seq_rows, norm_gain)
        query_raw = jnp.dot(normed, w_query, preferred_element_type=jnp.float32).astype(jnp.bfloat16)
        key_raw = jnp.dot(normed, w_key, preferred_element_type=jnp.float32).astype(jnp.bfloat16)
        values = jnp.dot(normed, w_value, preferred_element_type=jnp.float32).astype(jnp.bfloat16)
        gate_raw = jnp.dot(normed, w_gate, preferred_element_type=jnp.float32).astype(jnp.bfloat16)
        up_raw = jnp.dot(normed, w_up, preferred_element_type=jnp.float32).astype(jnp.bfloat16)
        query_rot = rope_rotate(query_raw.reshape(SEQ_LEN, N_HEADS, HEAD_DIM).astype(jnp.float32), cos_t[:, None, :], sin_t[:, None, :]).astype(jnp.bfloat16)
        key_f32 = rope_rotate(key_raw.astype(jnp.float32), cos_t, sin_t).astype(jnp.bfloat16).astype(jnp.float32)
        value_f32 = values.astype(jnp.float32)
        query_blocks = query_rot.reshape(n_blocks, q_block, N_HEADS, HEAD_DIM)

        def block_attn(block_args):
            query_rows, blk_start = block_args
            scores = jnp.einsum("qhe,te->qht", query_rows.astype(jnp.float32), key_f32) * score_scale
            query_index = blk_start + jnp.arange(q_block)
            causal_mask = key_index[None, None, :] <= query_index[:, None, None]
            scores = jnp.where(causal_mask, scores, -1e30)
            prob_rows = jax.nn.softmax(scores, axis=-1).astype(jnp.bfloat16)
            attn_rows = jnp.einsum("qht,te->qhe", prob_rows.astype(jnp.float32), value_f32)
            return attn_rows.astype(jnp.bfloat16)

        attn_out = lax.map(block_attn, (query_blocks, jnp.arange(n_blocks) * q_block))
        attn_out = attn_out.reshape(SEQ_LEN, N_HEADS * HEAD_DIM)
        gated_act = (jax.nn.silu(gate_raw.astype(jnp.float32)) * up_raw.astype(jnp.float32)).astype(jnp.bfloat16)
        branch = jnp.dot(attn_out, w_out, preferred_element_type=jnp.float32) + jnp.dot(gated_act, w_down, preferred_element_type=jnp.float32)
        return (seq_rows.astype(jnp.float32) + branch).astype(jnp.bfloat16)

    return lax.map(seq_layer, hidden)
```

```python
import functools

import jax
import jax.numpy as jnp
from jax import lax
from jax.experimental import pallas as pl
from jax.experimental.pallas import tpu as pltpu
from jax.sharding import PartitionSpec as P

MESH = pl.DeviceIdType.MESH
Q_BLOCK = 512
NORM_EPS = 1e-6
FF_CHUNKS = (512, 512, 256, 256)
M_TILE = 256


def rope_tables(positions, head_dim):
    inv_freq = 10000.0 ** (-jnp.arange(0, head_dim, 2, dtype=jnp.float32) / head_dim)
    angles = positions.astype(jnp.float32)[:, None] * inv_freq[None, :]
    angles = jnp.concatenate([angles, angles], axis=-1)
    return jnp.cos(angles), jnp.sin(angles)


def rope_rotate(vectors, cos_t, sin_t):
    half_dim = vectors.shape[-1] // 2
    rotated = jnp.concatenate([-vectors[..., half_dim:], vectors[..., :half_dim]], axis=-1)
    return vectors * cos_t + rotated * sin_t


def norm_kernel(n, rows_ref, *refs):
    gain_refs, out_ref, gain = refs[:n], refs[-2], refs[-1]
    me = lax.axis_index("fsdp")
    size = gain_refs[0].shape[1]

    @pl.when(pl.program_id(0) == 0)
    def _():
        for by, ref in enumerate(gain_refs):
            start = lax.rem(me + by, n) * size
            gain[:, pl.ds(pl.multiple_of(start, 128), size)] = ref[...]

    row_f32 = rows_ref[...].astype(jnp.float32)
    centered = row_f32 - jnp.mean(row_f32, axis=-1, keepdims=True)
    variance = jnp.mean(centered * centered, axis=-1, keepdims=True)
    out_ref[...] = (centered * lax.rsqrt(variance + NORM_EPS) * gain[...]).astype(jnp.bfloat16)


def layer_norm(n, rows, gain_pieces):
    seq_len, width = rows.shape
    tile = 128
    return pl.pallas_call(
        functools.partial(norm_kernel, n),
        grid=(seq_len // tile,),
        in_specs=[pl.BlockSpec((tile, width), lambda i: (i, 0))] + [pl.BlockSpec((1, width // n), lambda i: (0, 0))] * n,
        out_specs=pl.BlockSpec((tile, width), lambda i: (i, 0)),
        out_shape=jax.ShapeDtypeStruct(rows.shape, jnp.bfloat16),
        scratch_shapes=[pltpu.VMEM((1, width), jnp.float32)],
        compiler_params=pltpu.CompilerParams(dimension_semantics=("arbitrary",), vmem_limit_bytes=24 * 1024 * 1024),
        cost_estimate=pl.CostEstimate(flops=10000 * rows.size, bytes_accessed=4 * rows.size, transcendentals=0),
    )(rows, *[piece.reshape(1, -1) for piece in gain_pieces])


def causal_attention(query_rot, key_rot, values):
    seq_len, n_heads, head_dim = query_rot.shape
    q_block = min(Q_BLOCK, seq_len)
    score_scale = head_dim ** -0.5
    pieces = []
    for blk_idx in range(seq_len // q_block):
        blk_lo = blk_idx * q_block
        blk_hi = blk_lo + q_block
        scores = jnp.einsum("she,te->sht", query_rot[blk_lo:blk_hi], key_rot[:blk_hi], preferred_element_type=jnp.float32) * score_scale
        causal_mask = jnp.arange(blk_hi)[None, :] <= (blk_lo + jnp.arange(q_block))[:, None]
        scores = jnp.where(causal_mask[:, None, :], scores, -1e30)
        prob_rows = jax.nn.softmax(scores, axis=-1).astype(jnp.bfloat16)
        pieces.append(jnp.einsum("sht,te->she", prob_rows, values[:blk_hi], preferred_element_type=jnp.float32).astype(jnp.bfloat16))
    attn_out = jnp.concatenate(pieces, axis=0)
    return attn_out.reshape(seq_len, n_heads * head_dim)


def shift(n, by):
    return [(i, (i + by) % n) for i in range(n)]


def swap(n):
    return [(i, i ^ 1) for i in range(n)]


def ring_near(n, shard):
    return lax.ppermute(shard, "fsdp", shift(n, 2)), lax.ppermute(shard, "fsdp", shift(n, -2))


def ring_far(n, shard, near):
    from_left, from_right = near
    half = shard.shape[0] // 2
    far_lo = lax.ppermute(from_left[:half], "fsdp", shift(n, 2))
    far_hi = lax.ppermute(from_right[half:], "fsdp", shift(n, -2))
    pieces = []
    for chip, part, block in [(0, None, shard), (-1, None, from_left), (1, None, from_right), (2, 0, far_lo), (2, 1, far_hi)]:
        pieces.append((chip, 0, part, block))
        pieces.append((chip, 1, part, lax.ppermute(block, "fsdp", swap(n))))
    return pieces


def owner_of(me, n, chip, other):
    owner = lax.rem(me + 2 * chip + n, n)
    return owner + other * (1 - 2 * lax.rem(owner, 2))


def gathered_kernel(n, spec, width, halves, tile, act_ref, *refs):
    piece_refs, out_ref, weight, sems = refs[: len(spec)], refs[-3], refs[-2], refs[-1]
    me = lax.axis_index("fsdp")

    @pl.when(pl.program_id(0) == 0)
    def _():
        copies = []
        for idx, ((chip, other, part), ref) in enumerate(zip(spec, piece_refs)):
            rows = ref.shape[0]
            full = rows if part is None else 2 * rows
            start = owner_of(me, n, chip, other) * full + (rows if part else 0)
            dst = weight.at[pl.ds(pl.multiple_of(start, 128), rows), :]
            copies.append(pltpu.make_async_copy(ref, dst, sems.at[idx]))
        for copy in copies:
            copy.start()
        for copy in copies:
            copy.wait()

    if halves == 1:
        out_ref[...] = jnp.dot(act_ref[...], weight[...], preferred_element_type=jnp.float32).astype(jnp.bfloat16)
        return

    @pl.loop(0, width // tile)
    def _(step):
        lo = pl.multiple_of(step * tile, tile)
        gate = jnp.dot(act_ref[...], weight[:, pl.ds(lo, tile)], preferred_element_type=jnp.float32)
        up = jnp.dot(act_ref[...], weight[:, pl.ds(pl.multiple_of(width + lo, tile), tile)], preferred_element_type=jnp.float32)
        gate = gate.astype(jnp.bfloat16).astype(jnp.float32)
        up = up.astype(jnp.bfloat16).astype(jnp.float32)
        out_ref[:, pl.ds(lo, tile)] = (gate * jax.nn.sigmoid(gate) * up).astype(jnp.bfloat16)


def gathered_call(n, act, pieces, n_out, halves):
    seq_len, width = act.shape
    spec = tuple((chip, other, part) for chip, other, part, _ in pieces)
    blocks = [block for *_, block in pieces]
    return pl.pallas_call(
        functools.partial(gathered_kernel, n, spec, n_out, halves, 256),
        grid=(seq_len // M_TILE,),
        in_specs=[pl.BlockSpec((M_TILE, width), lambda i: (i, 0))] + [pl.BlockSpec(memory_space=pl.ANY)] * len(blocks),
        out_specs=pl.BlockSpec((M_TILE, n_out), lambda i: (i, 0)),
        out_shape=jax.ShapeDtypeStruct((seq_len, n_out), jnp.bfloat16),
        scratch_shapes=[pltpu.VMEM((width, n_out * halves), jnp.bfloat16), pltpu.SemaphoreType.DMA((len(blocks),))],
        compiler_params=pltpu.CompilerParams(dimension_semantics=("arbitrary",), vmem_limit_bytes=32 * 1024 * 1024),
        cost_estimate=pl.CostEstimate(
            flops=2 * seq_len * width * n_out * halves,
            bytes_accessed=2 * (seq_len * width + width * n_out * halves + seq_len * n_out),
            transcendentals=0,
        ),
    )(act, *blocks)


ROWS_L1 = 128
ROWS_L2 = 32
N_GROUPS = 8
BUBBLE = 3
STAGES = 9
PART_SLOTS = 5


def reduce_kernel(
    act_hbm, w2_hbm, rows_hbm, out_hbm,
    act, weight, part, whole, recv1, recv2, recv3, recv4, resid,
    send_sem, recv_sem, xsend_sem, xrecv_sem, load_sem, resid_sem, out_sem,
):
    n_fsdp = 8
    tp = lax.axis_index("tp")
    fs = lax.axis_index("fsdp")
    coord = {"y": lax.rem(tp, 4), "z": lax.div(tp, 4)}
    core = lax.rem(fs, 2)
    cols = w2_hbm.shape[-1]
    full = 2 * cols

    def at(axis, delta):
        moved = lax.rem(coord[axis] + delta + 4, 4)
        return {"tp": coord["z"] * 4 + moved if axis == "y" else moved * 4 + coord["y"]}

    right = {"fsdp": lax.rem(fs + 2, n_fsdp)}
    left = {"fsdp": lax.rem(fs + n_fsdp - 2, n_fsdp)}
    sib = {"fsdp": fs + 1 - 2 * core}

    barrier = pltpu.get_barrier_semaphore()
    peers = [at("y", 1), at("y", -1), at("z", 1), at("z", -1), right, left, sib]
    for peer in peers:
        pl.semaphore_signal(barrier, inc=1, device_id=peer, device_id_type=MESH)
    pl.semaphore_wait(barrier, len(peers))

    def xcopy(src, slot, peer):
        return pltpu.make_async_remote_copy(
            src_ref=src, dst_ref=weight.at[slot], send_sem=xsend_sem.at[slot], recv_sem=xrecv_sem.at[slot],
            device_id=peer, device_id_type=MESH)

    def first_sends():
        for half in range(2):
            xcopy(w2_hbm.at[half], 4 + half, right).start()
            xcopy(w2_hbm.at[half], 8 + half, left).start()
            xcopy(w2_hbm.at[half], 2 + half, sib).start()

    def x_wait_recv(slot):
        xcopy(weight.at[slot], slot, sib).wait_recv()

    first_sends()
    loads = [pltpu.make_async_copy(act_hbm, act, load_sem.at[0])]
    loads += [pltpu.make_async_copy(w2_hbm.at[half], weight.at[half], load_sem.at[1 + half]) for half in range(2)]
    for load in loads:
        load.start()
    for load in loads:
        load.wait()

    halves = [("y", "z"), ("z", "y")]

    def pslot(g):
        return lax.rem(g, PART_SLOTS)

    def block1(x, delta):
        k = lax.rem(coord[halves[x][0]] + delta + 4, 4)
        return pl.multiple_of(x * 4 * ROWS_L1 + k * ROWS_L1, ROWS_L1)

    def block2(x, delta):
        k = lax.rem(coord[halves[x][1]] + delta + 4, 4)
        return pl.multiple_of(block1(x, 0) + k * ROWS_L2, ROWS_L2)

    def offset(base, add):
        return pl.multiple_of(base + add, 16)

    def message(g, x, kind, src, dst, axis, delta):
        return pltpu.make_async_remote_copy(
            src_ref=src, dst_ref=dst, send_sem=send_sem.at[g, x, kind], recv_sem=recv_sem.at[g, x, kind],
            device_id=at(axis, delta), device_id_type=MESH)

    def scatter_far(g, x, level):
        block, axis, buf, rows, kind = (block1, halves[x][0], recv1, ROWS_L1, 0) if level == 1 else (block2, halves[x][1], recv3, ROWS_L2, 4)
        half = rows // 2
        far = block(x, 2)
        return [
            message(g, x, kind, part.at[pslot(g), pl.ds(far, half), :], buf.at[g, x, 0], axis, 1),
            message(g, x, kind + 1, part.at[pslot(g), pl.ds(offset(far, half), half), :], buf.at[g, x, 1], axis, -1),
        ]

    def scatter_near(g, x, level):
        block, axis, buf, rows, kind = (block1, halves[x][0], recv2, ROWS_L1, 2) if level == 1 else (block2, halves[x][1], recv4, ROWS_L2, 6)
        return [
            message(g, x, kind, part.at[pslot(g), pl.ds(block(x, 1), rows), :], buf.at[g, x, 0], axis, 1),
            message(g, x, kind + 1, part.at[pslot(g), pl.ds(block(x, -1), rows), :], buf.at[g, x, 1], axis, -1),
        ]

    def gather_near(g, x, level):
        block, axis, rows, kind = (block1, halves[x][0], ROWS_L1, 12) if level == 1 else (block2, halves[x][1], ROWS_L2, 8)
        mine = whole.at[g, pl.ds(block(x, 0), rows), :]
        return [message(g, x, kind, mine, mine, axis, 1), message(g, x, kind + 1, mine, mine, axis, -1)]

    def gather_far(g, x, level):
        block, axis, rows, kind = (block1, halves[x][0], ROWS_L1, 14) if level == 1 else (block2, halves[x][1], ROWS_L2, 10)
        half = rows // 2
        lo = whole.at[g, pl.ds(block(x, -1), half), :]
        hi = whole.at[g, pl.ds(offset(block(x, 1), half), half), :]
        return [message(g, x, kind, lo, lo, axis, 1), message(g, x, kind + 1, hi, hi, axis, -1)]

    def start(copies):
        for copy in copies:
            copy.start()

    def finish(copies):
        for copy in copies:
            copy.wait()

    def summed(g, row, rows, *refs):
        total = part[pslot(g), pl.ds(row, rows), :].astype(jnp.float32)
        for ref in refs:
            total = total + ref.astype(jnp.float32)
        return total.astype(jnp.bfloat16)

    def add_into(g, row, rows, *refs):
        part[pslot(g), pl.ds(row, rows), :] = summed(g, row, rows, *refs)

    def group_info(g):
        mid = jnp.logical_and(g >= 2, g < 6)
        i = g - 2
        odd = lax.rem(i + 2, 2)
        slot = jnp.where(g < 2, g, jnp.where(mid, 4 + 4 * odd + lax.div(i + 2, 2) - 1, g + 6))
        delta = jnp.where(g < 2, 0, jnp.where(mid, 2 * odd - 1, 2))
        half = jnp.where(mid, lax.div(i + 2, 2) - 1, lax.rem(g, 2))
        chip = lax.rem(lax.div(fs, 2) + delta + 4, 4)
        col_a = pl.multiple_of((chip * 2 + core) * full + half * cols, 128)
        col_b = pl.multiple_of((chip * 2 + 1 - core) * full + half * cols, 128)
        return slot, col_a, col_b

    def resid_copies(g):
        _, col_a, col_b = group_info(g)
        copies = []
        for x in range(2):
            for j, col in enumerate((col_a, col_b)):
                copies.append(pltpu.make_async_copy(
                    rows_hbm.at[pl.ds(block2(x, 0), ROWS_L2), pl.ds(col, cols)],
                    resid.at[g, x, :, pl.ds(j * cols, cols)], resid_sem.at[g, 2 * x + j]))
        return copies

    def out_copies(g):
        _, col_a, col_b = group_info(g)
        return [
            pltpu.make_async_copy(whole.at[g, :, pl.ds(j * cols, cols)], out_hbm.at[:, pl.ds(col, cols)], out_sem.at[g, j])
            for j, col in enumerate((col_a, col_b))
        ]

    def stage0(g):
        slot, _, _ = group_info(g)
        start(resid_copies(g))

        @pl.when(g == 2)
        def _():
            x_wait_recv(4)
            xcopy(weight.at[4], 6, sib).start()
            xcopy(weight.at[4], 12, right).start()
            x_wait_recv(8)
            xcopy(weight.at[8], 10, sib).start()

        @pl.when(g == 4)
        def _():
            x_wait_recv(5)
            xcopy(weight.at[5], 7, sib).start()
            x_wait_recv(9)
            xcopy(weight.at[9], 11, sib).start()
            xcopy(weight.at[9], 13, left).start()

        @pl.when(g == 6)
        def _():
            x_wait_recv(12)
            xcopy(weight.at[12], 14, sib).start()
            x_wait_recv(13)
            xcopy(weight.at[13], 15, sib).start()

        for known, known_slot in enumerate((2, 3, 6, 10, 7, 11, 14, 15)):
            @pl.when(g == known)
            def _():
                x_wait_recv(known_slot)

        @pl.loop(0, act.shape[0] // 256)
        def _(m):
            where = pl.ds(pl.multiple_of(m * 256, 256), 256)
            for j in range(2):
                value = jnp.dot(act[where, :], weight[slot + 2 * j], preferred_element_type=jnp.float32)
                part[pslot(g), where, j * cols : (j + 1) * cols] = value.astype(jnp.bfloat16)

        for x in range(2):
            start(scatter_far(g, x, 1))

    def scatter_mid(level):
        def run(g):
            buf = recv1 if level == 1 else recv3
            rows = ROWS_L1 if level == 1 else ROWS_L2
            block = block1 if level == 1 else block2
            for x in range(2):
                finish(scatter_far(g, x, level))
                add_into(g, block(x, 1), rows // 2, buf[g, x, 0])
                add_into(g, offset(block(x, -1), rows // 2), rows // 2, buf[g, x, 1])
            for x in range(2):
                start(scatter_near(g, x, level))
        return run

    def stage2(g):
        for x in range(2):
            finish(scatter_near(g, x, 1))
            add_into(g, block1(x, 0), ROWS_L1, recv2[g, x, 0], recv2[g, x, 1])
        for x in range(2):
            start(scatter_far(g, x, 2))

    def stage4(g):
        finish(resid_copies(g))
        for x in range(2):
            finish(scatter_near(g, x, 2))
            whole[g, pl.ds(block2(x, 0), ROWS_L2), :] = summed(g, block2(x, 0), ROWS_L2, recv4[g, x, 0], recv4[g, x, 1], resid[g, x])
        for x in range(2):
            start(gather_near(g, x, 2))

    def relay(done, then):
        def run(g):
            for x in range(2):
                finish(done[0](g, x, done[1]))
                start(then[0](g, x, then[1]))
        return run

    def stage8(g):
        for x in range(2):
            finish(gather_far(g, x, 1))
        start(out_copies(g))

    stages = [
        stage0, scatter_mid(1), stage2, scatter_mid(2), stage4,
        relay((gather_near, 2), (gather_far, 2)), relay((gather_far, 2), (gather_near, 1)),
        relay((gather_near, 1), (gather_far, 1)), stage8,
    ]

    @pl.loop(0, N_GROUPS + BUBBLE + STAGES - 1)
    def _(t):
        for s in reversed(range(STAGES)):
            d = t - s
            early = jnp.logical_and(d >= 0, d < 2)
            late = jnp.logical_and(d >= 2 + BUBBLE, d < N_GROUPS + BUBBLE)
            g = jnp.where(d < 2, d, d - BUBBLE)

            @pl.when(jnp.logical_or(early, late))
            def _():
                stages[s](g)

    @pl.loop(0, N_GROUPS)
    def _(g):
        finish(out_copies(g))

    for slot, peer in ((4, right), (5, right), (8, left), (9, left), (2, sib), (3, sib), (6, sib), (7, sib),
                       (10, sib), (11, sib), (12, right), (13, left), (14, sib), (15, sib)):
        xcopy(weight.at[slot], slot, peer).wait_send()


def second_product(act, w2_halves, rows):
    seq_len, depth = act.shape
    cols = w2_halves.shape[-1]
    wide = 2 * cols
    bf16 = jnp.bfloat16
    return pl.pallas_call(
        reduce_kernel,
        in_specs=[pl.BlockSpec(memory_space=pl.ANY)] * 3,
        out_specs=pl.BlockSpec(memory_space=pl.ANY),
        out_shape=jax.ShapeDtypeStruct(rows.shape, bf16),
        scratch_shapes=[
            pltpu.VMEM((seq_len, depth), bf16),
            pltpu.VMEM((16, depth, cols), bf16),
            pltpu.VMEM((PART_SLOTS, seq_len, wide), bf16),
            pltpu.VMEM((N_GROUPS, seq_len, wide), bf16),
            pltpu.VMEM((N_GROUPS, 2, 2, ROWS_L1 // 2, wide), bf16),
            pltpu.VMEM((N_GROUPS, 2, 2, ROWS_L1, wide), bf16),
            pltpu.VMEM((N_GROUPS, 2, 2, ROWS_L2 // 2, wide), bf16),
            pltpu.VMEM((N_GROUPS, 2, 2, ROWS_L2, wide), bf16),
            pltpu.VMEM((N_GROUPS, 2, ROWS_L2, wide), bf16),
            pltpu.SemaphoreType.DMA((N_GROUPS, 2, 16)),
            pltpu.SemaphoreType.DMA((N_GROUPS, 2, 16)),
            pltpu.SemaphoreType.DMA((16,)),
            pltpu.SemaphoreType.DMA((16,)),
            pltpu.SemaphoreType.DMA((3,)),
            pltpu.SemaphoreType.DMA((N_GROUPS, 4)),
            pltpu.SemaphoreType.DMA((N_GROUPS, 2)),
        ],
        compiler_params=pltpu.CompilerParams(collective_id=0, has_side_effects=True, vmem_limit_bytes=62 * 1024 * 1024),
        cost_estimate=pl.CostEstimate(
            flops=2 * seq_len * depth * rows.shape[1], bytes_accessed=2 * (seq_len * depth + 8 * depth * wide + 2 * rows.size), transcendentals=0),
    )(act, w2_halves, rows)


def solution(mesh):
    row_spec = P(("dp", "fsdp"), None, None)
    n_fsdp = mesh.shape["fsdp"]

    def local_layer(hidden, positions, norm_gain, w_query, w_key, w_value, w_gate, w_up, w_out, w_down):
        rows = hidden[0]
        seq_len = rows.shape[0]
        head_dim = w_key.shape[1]
        chunks = [jnp.concatenate([w_query, w_key, w_value], axis=1)]
        col = 0
        for width in FF_CHUNKS:
            chunks.append(jnp.concatenate([w_gate[:, col : col + width], w_up[:, col : col + width]], axis=1))
            col += width
        w2 = jnp.concatenate([w_out, w_down], axis=0)

        after = lax.optimization_barrier
        gains = [norm_gain]
        for by in range(1, n_fsdp):
            gains.append(lax.ppermute(norm_gain, "fsdp", shift(n_fsdp, -by)))
        near = [None] * len(chunks)
        chunks[0], _ = after((chunks[0], norm_gain))
        near[0] = ring_near(n_fsdp, chunks[0])
        chunks[1], _ = after((chunks[1], chunks[0]))
        near[1] = ring_near(n_fsdp, chunks[1])
        normed = layer_norm(n_fsdp, rows, gains)

        def ring_step(idx, done, nxt):
            *moved, _ = after((*near[idx], *([chunks[nxt]] if nxt else []), done))
            if nxt:
                chunks[nxt] = moved[2]
            pieces = ring_far(n_fsdp, chunks[idx], (moved[0], moved[1]))
            if nxt:
                near[nxt] = ring_near(n_fsdp, chunks[nxt])
            return pieces

        pieces0 = ring_step(0, normed, 2)
        pieces1 = ring_step(1, pieces0[0][3], 3)
        q_width = w_query.shape[1]
        qkv = gathered_call(n_fsdp, normed, pieces0, q_width + 2 * head_dim, 1)
        cos_t, sin_t = rope_tables(positions, head_dim)
        query_raw = qkv[:, :q_width].reshape(seq_len, -1, head_dim)
        key_raw = qkv[:, q_width : q_width + head_dim]
        values = qkv[:, q_width + head_dim :]
        query_rot = rope_rotate(query_raw.astype(jnp.float32), cos_t[:, None, :], sin_t[:, None, :]).astype(jnp.bfloat16)
        key_rot = rope_rotate(key_raw.astype(jnp.float32), cos_t, sin_t).astype(jnp.bfloat16)
        acts = [causal_attention(query_rot, key_rot, values)]
        pieces2 = ring_step(2, acts[0], 4)
        acts.append(gathered_call(n_fsdp, normed, pieces1, FF_CHUNKS[0], 2))
        pieces3 = ring_step(3, acts[1], None)
        acts.append(gathered_call(n_fsdp, normed, pieces2, FF_CHUNKS[1], 2))
        pieces4 = ring_step(4, acts[2], None)
        acts.append(gathered_call(n_fsdp, normed, pieces3, FF_CHUNKS[2], 2))
        acts.append(gathered_call(n_fsdp, normed, pieces4, FF_CHUNKS[3], 2))
        act = jnp.concatenate(acts, axis=1)

        depth = act.shape[1]
        w2_halves = w2.reshape(depth, 2, -1).transpose(1, 0, 2)
        return second_product(act, w2_halves, rows)[None]

    in_specs = (row_spec, P(None), P("fsdp"), P("fsdp", "tp"), P("fsdp", None), P("fsdp", None), P("fsdp", "tp"), P("fsdp", "tp"), P("tp", "fsdp"), P("tp", "fsdp"))
    return jax.shard_map(local_layer, mesh=mesh, in_specs=in_specs, out_specs=row_spec, check_vma=False)
```

```python
import functools

import jax
import jax.numpy as jnp
from jax import lax
from jax.experimental import pallas as pl
from jax.experimental.pallas import tpu as pltpu
from jax.sharding import PartitionSpec as P


MESH = pl.DeviceIdType.MESH
Q_BLOCK = 512
NORM_EPS = 1e-6
FF_CHUNKS = (512, 512, 256, 256)
M_TILE = 256
KERNEL_VMEM = 60 * 1024 * 1024


def rope_tables(positions, head_dim):
    inv_freq = 10000.0 ** (-jnp.arange(0, head_dim, 2, dtype=jnp.float32) / head_dim)
    angles = positions.astype(jnp.float32)[:, None] * inv_freq[None, :]
    angles = jnp.concatenate([angles, angles], axis=-1)
    return jnp.cos(angles), jnp.sin(angles)


def rope_rotate(vectors, cos_t, sin_t):
    half_dim = vectors.shape[-1] // 2
    rotated = jnp.concatenate([-vectors[..., half_dim:], vectors[..., :half_dim]], axis=-1)
    return vectors * cos_t + rotated * sin_t


def norm_kernel(n, rows_ref, *refs):
    gain_refs, out_ref, gain = refs[:n], refs[-2], refs[-1]
    me = lax.axis_index("fsdp")
    size = gain_refs[0].shape[1]

    @pl.when(pl.program_id(0) == 0)
    def _():
        for by, ref in enumerate(gain_refs):
            start = lax.rem(me + by, n) * size
            gain[:, pl.ds(pl.multiple_of(start, 128), size)] = ref[...]

    row_f32 = rows_ref[...].astype(jnp.float32)
    centered = row_f32 - jnp.mean(row_f32, axis=-1, keepdims=True)
    variance = jnp.mean(centered * centered, axis=-1, keepdims=True)
    out_ref[...] = (centered * lax.rsqrt(variance + NORM_EPS) * gain[...]).astype(jnp.bfloat16)


def layer_norm(n, rows, gain_pieces):
    seq_len, width = rows.shape
    tile = 128
    return pl.pallas_call(
        functools.partial(norm_kernel, n),
        grid=(seq_len // tile,),
        in_specs=[pl.BlockSpec((tile, width), lambda i: (i, 0))] + [pl.BlockSpec((1, width // n), lambda i: (0, 0))] * n,
        out_specs=pl.BlockSpec((tile, width), lambda i: (i, 0)),
        out_shape=jax.ShapeDtypeStruct(rows.shape, jnp.bfloat16),
        scratch_shapes=[pltpu.VMEM((1, width), jnp.float32)],
        compiler_params=pltpu.CompilerParams(dimension_semantics=("arbitrary",), vmem_limit_bytes=KERNEL_VMEM),
        cost_estimate=pl.CostEstimate(flops=10000 * rows.size, bytes_accessed=4 * rows.size, transcendentals=0),
    )(rows, *[piece.reshape(1, -1) for piece in gain_pieces])


def causal_attention(query_rot, key_rot, values):
    seq_len, n_heads, head_dim = query_rot.shape
    q_block = min(Q_BLOCK, seq_len)
    score_scale = head_dim ** -0.5
    pieces = []
    for blk_idx in range(seq_len // q_block):
        blk_lo = blk_idx * q_block
        blk_hi = blk_lo + q_block
        scores = jnp.einsum("she,te->sht", query_rot[blk_lo:blk_hi], key_rot[:blk_hi], preferred_element_type=jnp.float32) * score_scale
        causal_mask = jnp.arange(blk_hi)[None, :] <= (blk_lo + jnp.arange(q_block))[:, None]
        scores = jnp.where(causal_mask[:, None, :], scores, -1e30)
        prob_rows = jax.nn.softmax(scores, axis=-1).astype(jnp.bfloat16)
        pieces.append(jnp.einsum("sht,te->she", prob_rows, values[:blk_hi], preferred_element_type=jnp.float32).astype(jnp.bfloat16))
    attn_out = jnp.concatenate(pieces, axis=0)
    return attn_out.reshape(seq_len, n_heads * head_dim)


def shift(n, by):
    return [(i, (i + by) % n) for i in range(n)]


def swap(n):
    return [(i, i ^ 1) for i in range(n)]


def ring_near(n, shard):
    from_left = lax.ppermute(shard, "fsdp", shift(n, 2))
    from_right = lax.ppermute(shard, "fsdp", shift(n, -2))
    return from_left, from_right


def ring_far(n, near):
    from_left, from_right = near
    half = from_left.shape[0] // 2
    far_lo = lax.ppermute(from_left[:half], "fsdp", shift(n, 2))
    far_hi = lax.ppermute(from_right[half:], "fsdp", shift(n, -2))
    return far_lo, far_hi


def with_sibling(n, blocks, chips):
    pieces = []
    for (chip, part), block in zip(chips, blocks):
        pieces += [(chip, 0, part, block), (chip, 1, part, lax.ppermute(block, "fsdp", swap(n)))]
    return pieces


def owner_of(me, n, chip, other):
    owner = lax.rem(me + 2 * chip + n, n)
    return owner + other * (1 - 2 * lax.rem(owner, 2))


def gathered_kernel(n, spec, width, halves, tile, act_ref, *refs):
    piece_refs, out_ref, weight, sems = refs[: len(spec)], refs[-3], refs[-2], refs[-1]
    me = lax.axis_index("fsdp")

    @pl.when(pl.program_id(0) == 0)
    def _():
        copies = []
        for idx, ((chip, other, part, col), ref) in enumerate(zip(spec, piece_refs)):
            rows, columns = ref.shape
            full = rows if part is None else 2 * rows
            start = owner_of(me, n, chip, other) * full + (rows if part else 0)
            dst = weight.at[pl.ds(pl.multiple_of(start, 128), rows), pl.ds(col, columns)]
            copies.append(pltpu.make_async_copy(ref, dst, sems.at[idx]))
        for copy in copies:
            copy.start()
        for copy in copies:
            copy.wait()

    if halves == 1:
        out_ref[...] = jnp.dot(act_ref[...], weight[...], preferred_element_type=jnp.float32).astype(jnp.bfloat16)
        return

    @pl.loop(0, width // tile)
    def _(step):
        lo = pl.multiple_of(step * tile, tile)
        gate = jnp.dot(act_ref[...], weight[:, pl.ds(lo, tile)], preferred_element_type=jnp.float32)
        up = jnp.dot(act_ref[...], weight[:, pl.ds(pl.multiple_of(width + lo, tile), tile)], preferred_element_type=jnp.float32)
        gate = gate.astype(jnp.bfloat16).astype(jnp.float32)
        up = up.astype(jnp.bfloat16).astype(jnp.float32)
        out_ref[:, pl.ds(lo, tile)] = (gate * jax.nn.sigmoid(gate) * up).astype(jnp.bfloat16)


def gathered_call(n, act, groups, n_out, halves):
    seq_len, width = act.shape
    spec, blocks, col = [], [], 0
    for pieces in groups:
        spec += [(chip, other, part, col) for chip, other, part, _ in pieces]
        blocks += [block for *_, block in pieces]
        col += pieces[0][3].shape[1]
    return pl.pallas_call(
        functools.partial(gathered_kernel, n, spec, n_out, halves, 256),
        grid=(seq_len // M_TILE,),
        in_specs=[pl.BlockSpec((M_TILE, width), lambda i: (i, 0))] + [pl.BlockSpec(memory_space=pl.ANY)] * len(blocks),
        out_specs=pl.BlockSpec((M_TILE, n_out), lambda i: (i, 0)),
        out_shape=jax.ShapeDtypeStruct((seq_len, n_out), jnp.bfloat16),
        scratch_shapes=[pltpu.VMEM((width, n_out * halves), jnp.bfloat16), pltpu.SemaphoreType.DMA((len(blocks),))],
        compiler_params=pltpu.CompilerParams(dimension_semantics=("arbitrary",), vmem_limit_bytes=KERNEL_VMEM),
        cost_estimate=pl.CostEstimate(
            flops=2 * seq_len * width * n_out * halves,
            bytes_accessed=2 * (seq_len * width + width * n_out * halves + seq_len * n_out),
            transcendentals=0,
        ),
    )(act, *blocks)


ROWS_L1 = 128
ROWS_L2 = 32
N_GROUPS = 8
BUBBLE = 3
STAGES = 9
PART_SLOTS = 5


def reduce_kernel(n_acts, *refs):
    acts_hbm = refs[:n_acts]
    reduce_body(acts_hbm, *refs[n_acts:])


def reduce_body(
    acts_hbm, w2_hbm, rows_hbm, out_hbm,
    act, weight, part, whole, recv1, recv2, recv3, recv4, resid,
    send_sem, recv_sem, xsend_sem, xrecv_sem, load_sem, resid_sem, out_sem,
):
    n_fsdp = 8
    tp = lax.axis_index("tp")
    fs = lax.axis_index("fsdp")
    coord = {"y": lax.rem(tp, 4), "z": lax.div(tp, 4)}
    core = lax.rem(fs, 2)
    cols = w2_hbm.shape[-1]
    full = 2 * cols

    def at(axis, delta):
        moved = lax.rem(coord[axis] + delta + 4, 4)
        return {"tp": coord["z"] * 4 + moved if axis == "y" else moved * 4 + coord["y"]}

    right = {"fsdp": lax.rem(fs + 2, n_fsdp)}
    left = {"fsdp": lax.rem(fs + n_fsdp - 2, n_fsdp)}
    sib = {"fsdp": fs + 1 - 2 * core}

    barrier = pltpu.get_barrier_semaphore()
    peers = [at("y", 1), at("y", -1), at("z", 1), at("z", -1), right, left, sib]
    for peer in peers:
        pl.semaphore_signal(barrier, inc=1, device_id=peer, device_id_type=MESH)
    pl.semaphore_wait(barrier, len(peers))

    def xcopy(src, slot, peer):
        return pltpu.make_async_remote_copy(
            src_ref=src, dst_ref=weight.at[slot], send_sem=xsend_sem.at[slot], recv_sem=xrecv_sem.at[slot],
            device_id=peer, device_id_type=MESH)

    def first_sends():
        for half in range(2):
            xcopy(w2_hbm.at[half], 4 + half, right).start()
            xcopy(w2_hbm.at[half], 8 + half, left).start()
            xcopy(w2_hbm.at[half], 2 + half, sib).start()

    def x_wait_recv(slot):
        xcopy(weight.at[slot], slot, sib).wait_recv()

    first_sends()
    loads = [pltpu.make_async_copy(w2_hbm.at[half], weight.at[half], load_sem.at[half]) for half in range(2)]
    col = 0
    for idx, act_hbm in enumerate(acts_hbm):
        size = act_hbm.shape[1]
        loads.append(pltpu.make_async_copy(act_hbm, act.at[:, pl.ds(col, size)], load_sem.at[2 + idx]))
        col += size
    for load in loads:
        load.start()
    for load in loads:
        load.wait()

    halves = [("y", "z"), ("z", "y")]

    def pslot(g):
        return lax.rem(g, PART_SLOTS)

    def block1(x, delta):
        k = lax.rem(coord[halves[x][0]] + delta + 4, 4)
        return pl.multiple_of(x * 4 * ROWS_L1 + k * ROWS_L1, ROWS_L1)

    def block2(x, delta):
        k = lax.rem(coord[halves[x][1]] + delta + 4, 4)
        return pl.multiple_of(block1(x, 0) + k * ROWS_L2, ROWS_L2)

    def offset(base, add):
        return pl.multiple_of(base + add, 16)

    def message(g, x, kind, src, dst, axis, delta):
        return pltpu.make_async_remote_copy(
            src_ref=src, dst_ref=dst, send_sem=send_sem.at[g, x, kind], recv_sem=recv_sem.at[g, x, kind],
            device_id=at(axis, delta), device_id_type=MESH)

    def scatter_far(g, x, level):
        block, axis, buf, rows, kind = (block1, halves[x][0], recv1, ROWS_L1, 0) if level == 1 else (block2, halves[x][1], recv3, ROWS_L2, 4)
        half = rows // 2
        far = block(x, 2)
        return [
            message(g, x, kind, part.at[pslot(g), pl.ds(far, half), :], buf.at[g, x, 0], axis, 1),
            message(g, x, kind + 1, part.at[pslot(g), pl.ds(offset(far, half), half), :], buf.at[g, x, 1], axis, -1),
        ]

    def scatter_near(g, x, level):
        block, axis, buf, rows, kind = (block1, halves[x][0], recv2, ROWS_L1, 2) if level == 1 else (block2, halves[x][1], recv4, ROWS_L2, 6)
        return [
            message(g, x, kind, part.at[pslot(g), pl.ds(block(x, 1), rows), :], buf.at[g, x, 0], axis, 1),
            message(g, x, kind + 1, part.at[pslot(g), pl.ds(block(x, -1), rows), :], buf.at[g, x, 1], axis, -1),
        ]

    def gather_near(g, x, level):
        block, axis, rows, kind = (block1, halves[x][0], ROWS_L1, 12) if level == 1 else (block2, halves[x][1], ROWS_L2, 8)
        mine = whole.at[g, pl.ds(block(x, 0), rows), :]
        return [message(g, x, kind, mine, mine, axis, 1), message(g, x, kind + 1, mine, mine, axis, -1)]

    def gather_far(g, x, level):
        block, axis, rows, kind = (block1, halves[x][0], ROWS_L1, 14) if level == 1 else (block2, halves[x][1], ROWS_L2, 10)
        half = rows // 2
        lo = whole.at[g, pl.ds(block(x, -1), half), :]
        hi = whole.at[g, pl.ds(offset(block(x, 1), half), half), :]
        return [message(g, x, kind, lo, lo, axis, 1), message(g, x, kind + 1, hi, hi, axis, -1)]

    def start(copies):
        for copy in copies:
            copy.start()

    def finish(copies):
        for copy in copies:
            copy.wait()

    def summed(g, row, rows, *refs):
        total = part[pslot(g), pl.ds(row, rows), :].astype(jnp.float32)
        for ref in refs:
            total = total + ref.astype(jnp.float32)
        return total.astype(jnp.bfloat16)

    def add_into(g, row, rows, *refs):
        part[pslot(g), pl.ds(row, rows), :] = summed(g, row, rows, *refs)

    def group_info(g):
        mid = jnp.logical_and(g >= 2, g < 6)
        i = g - 2
        odd = lax.rem(i + 2, 2)
        slot = jnp.where(g < 2, g, jnp.where(mid, 4 + 4 * odd + lax.div(i + 2, 2) - 1, g + 6))
        delta = jnp.where(g < 2, 0, jnp.where(mid, 2 * odd - 1, 2))
        half = jnp.where(mid, lax.div(i + 2, 2) - 1, lax.rem(g, 2))
        chip = lax.rem(lax.div(fs, 2) + delta + 4, 4)
        col_a = pl.multiple_of((chip * 2 + core) * full + half * cols, 128)
        col_b = pl.multiple_of((chip * 2 + 1 - core) * full + half * cols, 128)
        return slot, col_a, col_b

    def resid_copies(g):
        _, col_a, col_b = group_info(g)
        copies = []
        for x in range(2):
            for j, col in enumerate((col_a, col_b)):
                copies.append(pltpu.make_async_copy(
                    rows_hbm.at[pl.ds(block2(x, 0), ROWS_L2), pl.ds(col, cols)],
                    resid.at[g, x, :, pl.ds(j * cols, cols)], resid_sem.at[g, 2 * x + j]))
        return copies

    def out_copies(g):
        _, col_a, col_b = group_info(g)
        return [
            pltpu.make_async_copy(whole.at[g, :, pl.ds(j * cols, cols)], out_hbm.at[:, pl.ds(col, cols)], out_sem.at[g, j])
            for j, col in enumerate((col_a, col_b))
        ]

    def stage0(g):
        slot, _, _ = group_info(g)
        start(resid_copies(g))

        @pl.when(g == 2)
        def _():
            x_wait_recv(4)
            xcopy(weight.at[4], 6, sib).start()
            xcopy(weight.at[4], 12, right).start()
            x_wait_recv(8)
            xcopy(weight.at[8], 10, sib).start()

        @pl.when(g == 4)
        def _():
            x_wait_recv(5)
            xcopy(weight.at[5], 7, sib).start()
            x_wait_recv(9)
            xcopy(weight.at[9], 11, sib).start()
            xcopy(weight.at[9], 13, left).start()

        @pl.when(g == 6)
        def _():
            x_wait_recv(12)
            xcopy(weight.at[12], 14, sib).start()
            x_wait_recv(13)
            xcopy(weight.at[13], 15, sib).start()

        for known, known_slot in enumerate((2, 3, 6, 10, 7, 11, 14, 15)):
            @pl.when(g == known)
            def _():
                x_wait_recv(known_slot)

        @pl.loop(0, act.shape[0] // 256)
        def _(m):
            where = pl.ds(pl.multiple_of(m * 256, 256), 256)
            for j in range(2):
                value = jnp.dot(act[where, :], weight[slot + 2 * j], preferred_element_type=jnp.float32)
                part[pslot(g), where, j * cols : (j + 1) * cols] = value.astype(jnp.bfloat16)

        for x in range(2):
            start(scatter_far(g, x, 1))

    def scatter_mid(level):
        def run(g):
            buf = recv1 if level == 1 else recv3
            rows = ROWS_L1 if level == 1 else ROWS_L2
            block = block1 if level == 1 else block2
            for x in range(2):
                finish(scatter_far(g, x, level))
                add_into(g, block(x, 1), rows // 2, buf[g, x, 0])
                add_into(g, offset(block(x, -1), rows // 2), rows // 2, buf[g, x, 1])
            for x in range(2):
                start(scatter_near(g, x, level))

        return run

    def stage2(g):
        for x in range(2):
            finish(scatter_near(g, x, 1))
            add_into(g, block1(x, 0), ROWS_L1, recv2[g, x, 0], recv2[g, x, 1])
        for x in range(2):
            start(scatter_far(g, x, 2))

    def stage4(g):
        finish(resid_copies(g))
        for x in range(2):
            finish(scatter_near(g, x, 2))
            whole[g, pl.ds(block2(x, 0), ROWS_L2), :] = summed(g, block2(x, 0), ROWS_L2, recv4[g, x, 0], recv4[g, x, 1], resid[g, x])
        for x in range(2):
            start(gather_near(g, x, 2))

    def relay(done, then):
        def run(g):
            for x in range(2):
                finish(done[0](g, x, done[1]))
                start(then[0](g, x, then[1]))

        return run

    def stage8(g):
        for x in range(2):
            finish(gather_far(g, x, 1))
        start(out_copies(g))

    stages = [
        stage0, scatter_mid(1), stage2, scatter_mid(2), stage4,
        relay((gather_near, 2), (gather_far, 2)), relay((gather_far, 2), (gather_near, 1)),
        relay((gather_near, 1), (gather_far, 1)), stage8,
    ]

    @pl.loop(0, N_GROUPS + BUBBLE + STAGES - 1)
    def _(t):
        for s in reversed(range(STAGES)):
            d = t - s
            early = jnp.logical_and(d >= 0, d < 2)
            late = jnp.logical_and(d >= 2 + BUBBLE, d < N_GROUPS + BUBBLE)
            g = jnp.where(d < 2, d, d - BUBBLE)

            @pl.when(jnp.logical_or(early, late))
            def _():
                stages[s](g)

    @pl.loop(0, N_GROUPS)
    def _(g):
        finish(out_copies(g))

    for slot, peer in ((4, right), (5, right), (8, left), (9, left), (2, sib), (3, sib), (6, sib), (7, sib),
                       (10, sib), (11, sib), (12, right), (13, left), (14, sib), (15, sib)):
        xcopy(weight.at[slot], slot, peer).wait_send()


def second_product(acts, w2_halves, rows):
    seq_len = rows.shape[0]
    depth = w2_halves.shape[1]
    cols = w2_halves.shape[-1]
    wide = 2 * cols
    bf16 = jnp.bfloat16
    return pl.pallas_call(
        functools.partial(reduce_kernel, len(acts)),
        in_specs=[pl.BlockSpec(memory_space=pl.ANY)] * (len(acts) + 2),
        out_specs=pl.BlockSpec(memory_space=pl.ANY),
        out_shape=jax.ShapeDtypeStruct(rows.shape, bf16),
        scratch_shapes=[
            pltpu.VMEM((seq_len, depth), bf16),
            pltpu.VMEM((16, depth, cols), bf16),
            pltpu.VMEM((PART_SLOTS, seq_len, wide), bf16),
            pltpu.VMEM((N_GROUPS, seq_len, wide), bf16),
            pltpu.VMEM((N_GROUPS, 2, 2, ROWS_L1 // 2, wide), bf16),
            pltpu.VMEM((N_GROUPS, 2, 2, ROWS_L1, wide), bf16),
            pltpu.VMEM((N_GROUPS, 2, 2, ROWS_L2 // 2, wide), bf16),
            pltpu.VMEM((N_GROUPS, 2, 2, ROWS_L2, wide), bf16),
            pltpu.VMEM((N_GROUPS, 2, ROWS_L2, wide), bf16),
            pltpu.SemaphoreType.DMA((N_GROUPS, 2, 16)),
            pltpu.SemaphoreType.DMA((N_GROUPS, 2, 16)),
            pltpu.SemaphoreType.DMA((16,)),
            pltpu.SemaphoreType.DMA((16,)),
            pltpu.SemaphoreType.DMA((2 + len(acts),)),
            pltpu.SemaphoreType.DMA((N_GROUPS, 4)),
            pltpu.SemaphoreType.DMA((N_GROUPS, 2)),
        ],
        compiler_params=pltpu.CompilerParams(collective_id=0, has_side_effects=True, vmem_limit_bytes=62 * 1024 * 1024),
        cost_estimate=pl.CostEstimate(
            flops=2 * seq_len * depth * rows.shape[1], bytes_accessed=2 * (seq_len * depth + 8 * depth * wide + 2 * rows.size), transcendentals=0),
    )(*acts, w2_halves, rows)


def solution(mesh):
    row_spec = P(("dp", "fsdp"), None, None)
    n_fsdp = mesh.shape["fsdp"]

    def layer(hidden, positions, norm_gain, w_query, w_key, w_value, w_gate, w_up, w_out, w_down):
        rows = hidden[0]
        seq_len = rows.shape[0]
        head_dim = w_key.shape[1]
        chunks = [w_query]
        key_value = jnp.concatenate([w_key, w_value], axis=1)
        col = 0
        for width in FF_CHUNKS:
            chunks.append(jnp.concatenate([w_gate[:, col : col + width], w_up[:, col : col + width]], axis=1))
            col += width
        w2 = jnp.concatenate([w_out, w_down], axis=0)

        w2_halves = w2.reshape(w2.shape[0], 2, -1).transpose(1, 0, 2)
        after = lax.optimization_barrier
        near = [None] * len(chunks)
        near[0] = ring_near(n_fsdp, chunks[0])
        gains = [norm_gain]
        for by in range(1, n_fsdp):
            gains.append(lax.ppermute(norm_gain, "fsdp", shift(n_fsdp, -by)))
        near_kv = ring_near(n_fsdp, key_value)
        chunks[1], _ = after((chunks[1], key_value))
        near[1] = ring_near(n_fsdp, chunks[1])
        normed = layer_norm(n_fsdp, rows, gains)
        lo, hi, _ = after((*near_kv, normed))
        far_kv = ring_far(n_fsdp, (lo, hi))
        kv_pieces = with_sibling(n_fsdp, [key_value, lo, hi], [(0, None), (-1, None), (1, None)])
        far = [None] * len(chunks)
        near_pieces = [None] * len(chunks)

        def ring_step(idx, done, nxt):
            *moved, _ = after((*near[idx], *([chunks[nxt]] if nxt else []), done))
            far[idx] = ring_far(n_fsdp, moved[:2])
            if nxt:
                chunks[nxt] = moved[2]
                near[nxt] = ring_near(n_fsdp, chunks[nxt])
            near_pieces[idx] = with_sibling(n_fsdp, [chunks[idx], *moved[:2]], [(0, None), (-1, None), (1, None)])

        def all_pieces(idx, done):
            lo, hi, _ = after((*far[idx], done))
            return near_pieces[idx] + with_sibling(n_fsdp, [lo, hi], [(2, 0), (2, 1)])

        def ffn(idx, done):
            pieces = all_pieces(idx, done)
            return gathered_call(n_fsdp, normed, [pieces], FF_CHUNKS[idx - 1], 2)

        ring_step(0, normed, 2)
        ring_step(1, near[0][0], 3)
        q_width = w_query.shape[1]
        pieces = all_pieces(0, normed)
        kv_pieces += with_sibling(n_fsdp, far_kv, [(2, 0), (2, 1)])
        acts_in, w2_halves = after((normed, w2_halves))
        qkv = gathered_call(n_fsdp, acts_in, [pieces, kv_pieces], q_width + 2 * head_dim, 1)
        cos_t, sin_t = rope_tables(positions, head_dim)
        query_raw = qkv[:, :q_width].reshape(seq_len, -1, head_dim)
        key_raw = qkv[:, q_width : q_width + head_dim]
        values = qkv[:, q_width + head_dim :]
        query_rot = rope_rotate(query_raw.astype(jnp.float32), cos_t[:, None, :], sin_t[:, None, :]).astype(jnp.bfloat16)
        key_rot = rope_rotate(key_raw.astype(jnp.float32), cos_t, sin_t).astype(jnp.bfloat16)
        acts = [causal_attention(query_rot, key_rot, values)]
        ring_step(2, acts[0], 4)
        acts.append(ffn(1, acts[0]))
        ring_step(3, acts[1], None)
        acts.append(ffn(2, acts[1]))
        ring_step(4, acts[2], None)
        acts.append(ffn(3, acts[2]))
        acts.append(ffn(4, acts[3]))
        return second_product(acts, w2_halves, rows)[None]

    in_specs = (row_spec, P(None), P("fsdp"), P("fsdp", "tp"), P("fsdp", None), P("fsdp", None), P("fsdp", "tp"), P("fsdp", "tp"), P("tp", "fsdp"), P("tp", "fsdp"))
    return jax.shard_map(layer, mesh=mesh, in_specs=in_specs, out_specs=row_spec, check_vma=False)
```

```python
import functools

import jax
import jax.numpy as jnp
import numpy as np
from jax import lax
from jax.experimental import pallas as pl
from jax.experimental.pallas import tpu as pltpu
from jax.sharding import PartitionSpec as P

MESH = pl.DeviceIdType.MESH
NORM_EPS = 1e-6


def rope_tables(positions, head_dim):
    inv_freq = 10000.0 ** (-jnp.arange(0, head_dim, 2, dtype=jnp.float32) / head_dim)
    angles = positions.astype(jnp.float32)[:, None] * inv_freq[None, :]
    angles = jnp.concatenate([angles, angles], axis=-1)
    return jnp.cos(angles), jnp.sin(angles)


FF_TILE = 256


def first_kernel(
    rows_hbm, gain_hbm, wq_hbm, wk_hbm, wv_hbm, wg_hbm, wu_hbm, cos_ref, sin_ref, pick_ref, pick_rot_ref, place_ref,
    attn_hbm, z_hbm,
    act, gains, wq, wk, wv, wff, q_heads, k_rot, values, zbuf,
    send_sem, recv_sem, gain_send, gain_recv, load_sem, act_sem, out_sem,
):
    n = 8
    fs = lax.axis_index("fsdp")
    core = lax.rem(fs, 2)
    chip = lax.div(fs, 2)
    depth = wq_hbm.shape[0]
    half = depth // 2
    seq_len = rows_hbm.shape[0]
    n_chunks = wg_hbm.shape[1] // FF_TILE

    def device(by_chip, other):
        c = core if not other else 1 - core
        return lax.rem(chip + by_chip + 4, 4) * 2 + c

    right, left, sib = ({"fsdp": device(*p)} for p in ((1, 0), (-1, 0), (0, 1)))
    places = [(0, 0), (0, 1), (-1, 0), (-1, 1), (1, 0), (1, 1), (2, 0), (2, 1)]

    barrier = pltpu.get_barrier_semaphore()
    for by in range(1, n):
        pl.semaphore_signal(barrier, inc=1, device_id={"fsdp": lax.rem(fs + by, n)}, device_id_type=MESH)
    pl.semaphore_wait(barrier, n - 1)

    def qkv_streams():
        return [(0, wq_hbm, lambda at: wq.at[at, :]), (1, wk_hbm, lambda at: wk.at[at, :]), (2, wv_hbm, lambda at: wv.at[at, :])]

    def ff_streams(c):
        cols = pl.ds(pl.multiple_of(c * FF_TILE, FF_TILE), FF_TILE)
        return [
            (3 + 2 * c, wg_hbm.at[:, cols], lambda at: wff.at[c, at, pl.ds(0, FF_TILE)]),
            (4 + 2 * c, wu_hbm.at[:, cols], lambda at: wff.at[c, at, pl.ds(FF_TILE, FF_TILE)]),
        ]

    messages = [
        (2 * depth, depth, None, right), (4 * depth, depth, None, left),
        (6 * depth, half, 2 * depth, right), (6 * depth + half, half, 4 * depth + half, left),
        (depth, depth, None, sib), (3 * depth, depth, 2 * depth, sib), (5 * depth, depth, 4 * depth, sib),
        (7 * depth, half, 6 * depth, sib), (7 * depth + half, half, 6 * depth + half, sib),
    ]

    def message(stream, idx):
        row, own, gathered = stream
        dst, size, src, peer = messages[idx]
        return pltpu.make_async_remote_copy(
            src_ref=own if src is None else gathered(pl.ds(src, size)), dst_ref=gathered(pl.ds(dst, size)),
            send_sem=send_sem.at[row, idx], recv_sem=recv_sem.at[row, idx], device_id=peer, device_id_type=MESH)

    def own_load(stream):
        row, own, gathered = stream
        return pltpu.make_async_copy(own, gathered(pl.ds(0, depth)), load_sem.at[row])

    def send(streams, *idxs):
        for idx in idxs:
            for stream in streams:
                message(stream, idx).start()

    def receive(streams, *idxs):
        for idx in idxs:
            for stream in streams:
                message(stream, idx).wait_recv()

    def begin(streams):
        send(streams, 0, 1, 4)
        for stream in streams:
            own_load(stream).start()

    def pass_on(streams):
        receive(streams, 0, 1)
        send(streams, 2, 3, 5, 6)

    def complete(streams):
        receive(streams, 2, 3)
        send(streams, 7, 8)
        for stream in streams:
            own_load(stream).wait()
        receive(streams, 4, 5, 6, 7, 8)

    def gain_copy(slot):
        by_chip, other = places[slot]
        return pltpu.make_async_remote_copy(
            src_ref=gain_hbm, dst_ref=gains.at[slot], send_sem=gain_send.at[slot], recv_sem=gain_recv.at[slot],
            device_id={"fsdp": device(-by_chip, other)}, device_id_type=MESH)

    for slot in range(1, n):
        gain_copy(slot).start()
    begin(qkv_streams())
    begin(ff_streams(0))
    own_gain = pltpu.make_async_copy(gain_hbm, gains.at[0], gain_send.at[0])
    own_gain.start()
    blocks = []
    for slot, place in enumerate(places):
        cols = pl.ds(pl.multiple_of(device(*place) * depth, 128), depth)
        blocks.append(pltpu.make_async_copy(rows_hbm.at[:, cols], act.at[:, pl.ds(slot * depth, depth)], act_sem.at[slot]))
    for block in blocks:
        block.start()
    own_gain.wait()
    for slot in range(1, n):
        gain_copy(slot).wait()
    for block in blocks:
        block.wait()

    @pl.loop(0, seq_len // 16)
    def _(r):
        where = pl.ds(pl.multiple_of(r * 16, 16), 16)
        row_f32 = act[where, :].astype(jnp.float32)
        centered = row_f32 - jnp.mean(row_f32, axis=-1, keepdims=True)
        variance = jnp.mean(centered * centered, axis=-1, keepdims=True)
        scaled = centered * lax.rsqrt(variance + NORM_EPS)
        for slot in range(n):
            cols = slice(slot * depth, (slot + 1) * depth)
            act[where, cols] = (scaled[:, cols] * gains[slot]).astype(jnp.bfloat16)

    pass_on(qkv_streams())
    begin(ff_streams(1))
    pass_on(ff_streams(0))
    begin(ff_streams(2))
    complete(qkv_streams())

    n_heads, _, head_dim = pick_ref.shape
    q_block = 256

    @pl.loop(0, seq_len // q_block)
    def _(m):
        where = pl.ds(pl.multiple_of(m * q_block, q_block), q_block)
        cos_t, sin_t = cos_ref[where, :], sin_ref[where, :]
        dot = functools.partial(jnp.dot, preferred_element_type=jnp.float32)
        query_raw = dot(act[where, :], wq[...]).astype(jnp.bfloat16)
        for h in range(n_heads):
            rotated = dot(query_raw, pick_ref[h]) * cos_t + dot(query_raw, pick_rot_ref[h]) * sin_t
            q_heads[h, where, :] = rotated.astype(jnp.bfloat16)
        key_raw = dot(act[where, :], wk[...]).astype(jnp.bfloat16)
        key_turned = dot(key_raw, pick_rot_ref[0, 0:head_dim, :])
        k_rot[where, :] = (key_raw.astype(jnp.float32) * cos_t + key_turned * sin_t).astype(jnp.bfloat16)
        values[where, :] = dot(act[where, :], wv[...]).astype(jnp.bfloat16)

    for idx in range(9):
        message(qkv_streams()[0], idx).wait_send()
    pass_on(ff_streams(1))
    begin(ff_streams(3))

    score_scale = head_dim ** -0.5
    for blk in range(seq_len // q_block):
        lo, hi = blk * q_block, (blk + 1) * q_block
        causal_mask = lax.broadcasted_iota(jnp.int32, (q_block, hi), 1) <= lo + lax.broadcasted_iota(jnp.int32, (q_block, hi), 0)
        wq[lo:hi, :] = jnp.zeros((q_block, wq.shape[1]), jnp.bfloat16)

        @pl.loop(0, n_heads)
        def _(h):
            scores = lax.dot_general(q_heads[h, lo:hi, :], k_rot[0:hi, :], (((1,), (1,)), ((), ())), preferred_element_type=jnp.float32) * score_scale
            scores = jnp.where(causal_mask, scores, -1e30)
            weights = jnp.exp(scores - jnp.max(scores, axis=-1, keepdims=True))
            prob_rows = (weights / jnp.sum(weights, axis=-1, keepdims=True)).astype(jnp.bfloat16)
            out = jnp.dot(prob_rows, values[0:hi, :], preferred_element_type=jnp.float32).astype(jnp.bfloat16)
            placed = jnp.dot(out, place_ref[h], preferred_element_type=jnp.float32).astype(jnp.bfloat16)
            wq[lo:hi, :] = wq[lo:hi, :] + placed

    attn_out = pltpu.make_async_copy(wq.at[pl.ds(0, seq_len), :], attn_hbm, out_sem.at[n_chunks])
    attn_out.start()

    def z_out(c):
        cols = pl.ds(pl.multiple_of(c * FF_TILE, FF_TILE), FF_TILE)
        return pltpu.make_async_copy(zbuf.at[lax.rem(c, 2)], z_hbm.at[:, cols], out_sem.at[c])

    @pl.loop(0, n_chunks)
    def _(c):
        @pl.when(c + 2 < n_chunks)
        def _():
            pass_on(ff_streams(c + 2))

        @pl.when(c + 4 < n_chunks)
        def _():
            begin(ff_streams(c + 4))

        complete(ff_streams(c))

        @pl.when(c >= 2)
        def _():
            z_out(c - 2).wait()

        @pl.loop(0, seq_len // 256)
        def _(m):
            where = pl.ds(pl.multiple_of(m * 256, 256), 256)
            both = jnp.dot(act[where, :], wff[c], preferred_element_type=jnp.float32)
            gate = both[:, :FF_TILE].astype(jnp.bfloat16).astype(jnp.float32)
            up = both[:, FF_TILE:].astype(jnp.bfloat16).astype(jnp.float32)
            zbuf[lax.rem(c, 2), where, :] = (gate * jax.nn.sigmoid(gate) * up).astype(jnp.bfloat16)

        z_out(c).start()

    for c in (n_chunks - 2, n_chunks - 1):
        z_out(c).wait()
    attn_out.wait()
    for stream in qkv_streams()[1:]:
        for idx in range(9):
            message(stream, idx).wait_send()

    @pl.loop(0, n_chunks)
    def _(c):
        for stream in ff_streams(c):
            for idx in range(9):
                message(stream, idx).wait_send()


def first_products(rows, norm_gain, w_query, w_key, w_value, w_gate, w_up, cos_t, sin_t):
    seq_len, width = rows.shape
    q_width, head_dim, ff = w_query.shape[1], w_key.shape[1], w_gate.shape[1]
    n_heads = q_width // head_dim
    n_chunks = ff // FF_TILE
    bf16 = jnp.bfloat16
    feature = np.arange(head_dim)
    head = np.arange(n_heads)[:, None, None] * head_dim
    source = np.arange(q_width)[None, :, None]
    one_hot = np.where(source == head + feature, 1.0, 0.0)
    turned = np.where(feature < head_dim // 2, feature + head_dim // 2, feature - head_dim // 2)
    sign = np.where(feature < head_dim // 2, -1.0, 1.0)
    pick = jnp.asarray(one_hot, bf16)
    pick_rot = jnp.asarray(np.where(source == head + turned, sign, 0.0), bf16)
    place = jnp.asarray(one_hot.transpose(0, 2, 1), bf16)
    hbm = pl.BlockSpec(memory_space=pl.ANY)
    vmem = pl.BlockSpec(memory_space=pltpu.VMEM)
    return pl.pallas_call(
        first_kernel,
        in_specs=[hbm] * 7 + [vmem] * 5,
        out_specs=[hbm, hbm],
        out_shape=[jax.ShapeDtypeStruct((seq_len, q_width), bf16), jax.ShapeDtypeStruct((seq_len, ff), bf16)],
        scratch_shapes=[
            pltpu.VMEM((seq_len, width), bf16),
            pltpu.VMEM((8, 1, width // 8), jnp.float32),
            pltpu.VMEM((width, q_width), bf16),
            pltpu.VMEM((width, head_dim), bf16),
            pltpu.VMEM((width, head_dim), bf16),
            pltpu.VMEM((n_chunks, width, 2 * FF_TILE), bf16),
            pltpu.VMEM((n_heads, seq_len, head_dim), bf16),
            pltpu.VMEM((seq_len, head_dim), bf16),
            pltpu.VMEM((seq_len, head_dim), bf16),
            pltpu.VMEM((2, seq_len, FF_TILE), bf16),
            pltpu.SemaphoreType.DMA((3 + 2 * n_chunks, 9)),
            pltpu.SemaphoreType.DMA((3 + 2 * n_chunks, 9)),
            pltpu.SemaphoreType.DMA((8,)),
            pltpu.SemaphoreType.DMA((8,)),
            pltpu.SemaphoreType.DMA((3 + 2 * n_chunks,)),
            pltpu.SemaphoreType.DMA((8,)),
            pltpu.SemaphoreType.DMA((n_chunks + 1,)),
        ],
        compiler_params=pltpu.CompilerParams(collective_id=1, has_side_effects=True, vmem_limit_bytes=67043328),
    )(rows, norm_gain.reshape(1, -1), w_query, w_key, w_value, w_gate, w_up, cos_t, sin_t, pick, pick_rot, place)


ROWS_L1 = 128
ROWS_L2 = 32
N_GROUPS = 8
BUBBLE = 3
STAGES = 9
PART_SLOTS = 5


def reduce_kernel(n_acts, *refs):
    acts_hbm = refs[:n_acts]
    reduce_body(acts_hbm, *refs[n_acts:])


def reduce_body(
    acts_hbm, wo_hbm, wd_hbm, rows_hbm, out_hbm,
    act, weight, part, whole, recv1, recv2, recv3, recv4, resid,
    send_sem, recv_sem, xsend_sem, xrecv_sem, load_sem, resid_sem, out_sem,
):
    n_fsdp = 8
    tp = lax.axis_index("tp")
    fs = lax.axis_index("fsdp")
    coord = {"y": lax.rem(tp, 4), "z": lax.div(tp, 4)}
    core = lax.rem(fs, 2)
    full = wo_hbm.shape[1]
    cols = full // 2
    split = wo_hbm.shape[0]

    def at(axis, delta):
        moved = lax.rem(coord[axis] + delta + 4, 4)
        return {"tp": coord["z"] * 4 + moved if axis == "y" else moved * 4 + coord["y"]}

    right = {"fsdp": lax.rem(fs + 2, n_fsdp)}
    left = {"fsdp": lax.rem(fs + n_fsdp - 2, n_fsdp)}
    sib = {"fsdp": fs + 1 - 2 * core}

    barrier = pltpu.get_barrier_semaphore()
    peers = [at("y", 1), at("y", -1), at("z", 1), at("z", -1), right, left, sib]
    for peer in peers:
        pl.semaphore_signal(barrier, inc=1, device_id=peer, device_id_type=MESH)
    pl.semaphore_wait(barrier, len(peers))

    def xcopy(src, slot, peer):
        return pltpu.make_async_remote_copy(
            src_ref=src, dst_ref=weight.at[slot], send_sem=xsend_sem.at[slot, 0], recv_sem=xrecv_sem.at[slot, 0],
            device_id=peer, device_id_type=MESH)

    def own_parts(half):
        where = pl.ds(half * cols, cols)
        return [(wo_hbm.at[:, where], pl.ds(0, split)), (wd_hbm.at[:, where], pl.ds(split, wd_hbm.shape[0]))]

    def own_copies(slot, peer):
        return [
            pltpu.make_async_remote_copy(
                src_ref=src, dst_ref=weight.at[slot, at], send_sem=xsend_sem.at[slot, j], recv_sem=xrecv_sem.at[slot, j],
                device_id=peer, device_id_type=MESH)
            for j, (src, at) in enumerate(own_parts(slot % 2))
        ]

    own_sends = [(4, right), (8, left), (2, sib), (5, right), (9, left), (3, sib)]
    relays = [(6, sib), (7, sib), (10, sib), (11, sib), (12, right), (13, left), (14, sib), (15, sib)]

    def x_wait_recv(slot):
        if slot in (2, 3, 4, 5, 8, 9):
            for copy in own_copies(slot, sib):
                copy.wait_recv()
        else:
            xcopy(weight.at[slot], slot, sib).wait_recv()

    for slot, peer in own_sends:
        for copy in own_copies(slot, peer):
            copy.start()
    loads = []
    for half in range(2):
        for j, (src, part_rows) in enumerate(own_parts(half)):
            loads.append(pltpu.make_async_copy(src, weight.at[half, part_rows], load_sem.at[2 * half + j]))
    col = 0
    for idx, act_hbm in enumerate(acts_hbm):
        size = act_hbm.shape[1]
        loads.append(pltpu.make_async_copy(act_hbm, act.at[:, pl.ds(col, size)], load_sem.at[4 + idx]))
        col += size
    for load in loads:
        load.start()
    for load in loads:
        load.wait()

    halves = [("y", "z"), ("z", "y")]

    def pslot(g):
        return lax.rem(g, PART_SLOTS)

    def block1(x, delta):
        k = lax.rem(coord[halves[x][0]] + delta + 4, 4)
        return pl.multiple_of(x * 4 * ROWS_L1 + k * ROWS_L1, ROWS_L1)

    def block2(x, delta):
        k = lax.rem(coord[halves[x][1]] + delta + 4, 4)
        return pl.multiple_of(block1(x, 0) + k * ROWS_L2, ROWS_L2)

    def offset(base, add):
        return pl.multiple_of(base + add, 16)

    def message(g, x, kind, src, dst, axis, delta):
        return pltpu.make_async_remote_copy(
            src_ref=src, dst_ref=dst, send_sem=send_sem.at[g, x, kind], recv_sem=recv_sem.at[g, x, kind],
            device_id=at(axis, delta), device_id_type=MESH)

    def scatter_far(g, x, level):
        block, axis, buf, rows, kind = (block1, halves[x][0], recv1, ROWS_L1, 0) if level == 1 else (block2, halves[x][1], recv3, ROWS_L2, 4)
        half = rows // 2
        far = block(x, 2)
        return [
            message(g, x, kind, part.at[pslot(g), pl.ds(far, half), :], buf.at[g, x, 0], axis, 1),
            message(g, x, kind + 1, part.at[pslot(g), pl.ds(offset(far, half), half), :], buf.at[g, x, 1], axis, -1),
        ]

    def scatter_near(g, x, level):
        block, axis, buf, rows, kind = (block1, halves[x][0], recv2, ROWS_L1, 2) if level == 1 else (block2, halves[x][1], recv4, ROWS_L2, 6)
        return [
            message(g, x, kind, part.at[pslot(g), pl.ds(block(x, 1), rows), :], buf.at[g, x, 0], axis, 1),
            message(g, x, kind + 1, part.at[pslot(g), pl.ds(block(x, -1), rows), :], buf.at[g, x, 1], axis, -1),
        ]

    def gather_near(g, x, level):
        block, axis, rows, kind = (block1, halves[x][0], ROWS_L1, 12) if level == 1 else (block2, halves[x][1], ROWS_L2, 8)
        mine = whole.at[g, pl.ds(block(x, 0), rows), :]
        return [message(g, x, kind, mine, mine, axis, 1), message(g, x, kind + 1, mine, mine, axis, -1)]

    def gather_far(g, x, level):
        block, axis, rows, kind = (block1, halves[x][0], ROWS_L1, 14) if level == 1 else (block2, halves[x][1], ROWS_L2, 10)
        half = rows // 2
        lo = whole.at[g, pl.ds(block(x, -1), half), :]
        hi = whole.at[g, pl.ds(offset(block(x, 1), half), half), :]
        return [message(g, x, kind, lo, lo, axis, 1), message(g, x, kind + 1, hi, hi, axis, -1)]

    def start(copies):
        for copy in copies:
            copy.start()

    def finish(copies):
        for copy in copies:
            copy.wait()

    def summed(g, row, rows, *refs):
        total = part[pslot(g), pl.ds(row, rows), :].astype(jnp.float32)
        for ref in refs:
            total = total + ref.astype(jnp.float32)
        return total.astype(jnp.bfloat16)

    def add_into(g, row, rows, *refs):
        part[pslot(g), pl.ds(row, rows), :] = summed(g, row, rows, *refs)

    def group_info(g):
        mid = jnp.logical_and(g >= 2, g < 6)
        i = g - 2
        odd = lax.rem(i + 2, 2)
        slot = jnp.where(g < 2, g, jnp.where(mid, 4 + 4 * odd + lax.div(i + 2, 2) - 1, g + 6))
        delta = jnp.where(g < 2, 0, jnp.where(mid, 2 * odd - 1, 2))
        half = jnp.where(mid, lax.div(i + 2, 2) - 1, lax.rem(g, 2))
        chip = lax.rem(lax.div(fs, 2) + delta + 4, 4)
        col_a = pl.multiple_of((chip * 2 + core) * full + half * cols, 128)
        col_b = pl.multiple_of((chip * 2 + 1 - core) * full + half * cols, 128)
        return slot, col_a, col_b

    def resid_copies(g):
        _, col_a, col_b = group_info(g)
        copies = []
        for x in range(2):
            for j, col in enumerate((col_a, col_b)):
                copies.append(pltpu.make_async_copy(
                    rows_hbm.at[pl.ds(block2(x, 0), ROWS_L2), pl.ds(col, cols)],
                    resid.at[g, x, :, pl.ds(j * cols, cols)], resid_sem.at[g, 2 * x + j]))
        return copies

    def out_copies(g):
        _, col_a, col_b = group_info(g)
        return [
            pltpu.make_async_copy(whole.at[g, :, pl.ds(j * cols, cols)], out_hbm.at[:, pl.ds(col, cols)], out_sem.at[g, j])
            for j, col in enumerate((col_a, col_b))
        ]

    def stage0(g):
        slot, _, _ = group_info(g)
        start(resid_copies(g))

        @pl.when(g == 2)
        def _():
            x_wait_recv(4)
            xcopy(weight.at[4], 6, sib).start()
            xcopy(weight.at[4], 12, right).start()
            x_wait_recv(8)
            xcopy(weight.at[8], 10, sib).start()

        @pl.when(g == 4)
        def _():
            x_wait_recv(5)
            xcopy(weight.at[5], 7, sib).start()
            x_wait_recv(9)
            xcopy(weight.at[9], 11, sib).start()
            xcopy(weight.at[9], 13, left).start()

        @pl.when(g == 6)
        def _():
            x_wait_recv(12)
            xcopy(weight.at[12], 14, sib).start()
            x_wait_recv(13)
            xcopy(weight.at[13], 15, sib).start()

        for known, known_slot in enumerate((2, 3, 6, 10, 7, 11, 14, 15)):
            @pl.when(g == known)
            def _():
                x_wait_recv(known_slot)

        @pl.loop(0, act.shape[0] // 256)
        def _(m):
            where = pl.ds(pl.multiple_of(m * 256, 256), 256)
            for j in range(2):
                value = jnp.dot(act[where, :], weight[slot + 2 * j], preferred_element_type=jnp.float32)
                part[pslot(g), where, j * cols : (j + 1) * cols] = value.astype(jnp.bfloat16)

        for x in range(2):
            start(scatter_far(g, x, 1))

    def scatter_mid(level):
        def run(g):
            buf = recv1 if level == 1 else recv3
            rows = ROWS_L1 if level == 1 else ROWS_L2
            block = block1 if level == 1 else block2
            for x in range(2):
                finish(scatter_far(g, x, level))
                add_into(g, block(x, 1), rows // 2, buf[g, x, 0])
                add_into(g, offset(block(x, -1), rows // 2), rows // 2, buf[g, x, 1])
            for x in range(2):
                start(scatter_near(g, x, level))
        return run

    def stage2(g):
        for x in range(2):
            finish(scatter_near(g, x, 1))
            add_into(g, block1(x, 0), ROWS_L1, recv2[g, x, 0], recv2[g, x, 1])
        for x in range(2):
            start(scatter_far(g, x, 2))

    def stage4(g):
        finish(resid_copies(g))
        for x in range(2):
            finish(scatter_near(g, x, 2))
            whole[g, pl.ds(block2(x, 0), ROWS_L2), :] = summed(g, block2(x, 0), ROWS_L2, recv4[g, x, 0], recv4[g, x, 1], resid[g, x])
        for x in range(2):
            start(gather_near(g, x, 2))

    def relay(done, then):
        def run(g):
            for x in range(2):
                finish(done[0](g, x, done[1]))
                start(then[0](g, x, then[1]))
        return run

    def stage8(g):
        for x in range(2):
            finish(gather_far(g, x, 1))
        start(out_copies(g))

    stages = [
        stage0, scatter_mid(1), stage2, scatter_mid(2), stage4,
        relay((gather_near, 2), (gather_far, 2)), relay((gather_far, 2), (gather_near, 1)),
        relay((gather_near, 1), (gather_far, 1)), stage8,
    ]

    @pl.loop(0, N_GROUPS + BUBBLE + STAGES - 1)
    def _(t):
        for s in reversed(range(STAGES)):
            d = t - s
            early = jnp.logical_and(d >= 0, d < 2)
            late = jnp.logical_and(d >= 2 + BUBBLE, d < N_GROUPS + BUBBLE)
            g = jnp.where(d < 2, d, d - BUBBLE)

            @pl.when(jnp.logical_or(early, late))
            def _():
                stages[s](g)

    @pl.loop(0, N_GROUPS)
    def _(g):
        finish(out_copies(g))

    for slot, peer in own_sends:
        for copy in own_copies(slot, peer):
            copy.wait_send()
    for slot, peer in relays:
        xcopy(weight.at[slot], slot, peer).wait_send()


def second_product(acts, w_out, w_down, rows):
    seq_len = rows.shape[0]
    depth = w_out.shape[0] + w_down.shape[0]
    wide = w_out.shape[1]
    cols = wide // 2
    bf16 = jnp.bfloat16
    return pl.pallas_call(
        functools.partial(reduce_kernel, len(acts)),
        in_specs=[pl.BlockSpec(memory_space=pl.ANY)] * (len(acts) + 3),
        out_specs=pl.BlockSpec(memory_space=pl.ANY),
        out_shape=jax.ShapeDtypeStruct(rows.shape, bf16),
        scratch_shapes=[
            pltpu.VMEM((seq_len, depth), bf16),
            pltpu.VMEM((16, depth, cols), bf16),
            pltpu.VMEM((PART_SLOTS, seq_len, wide), bf16),
            pltpu.VMEM((N_GROUPS, seq_len, wide), bf16),
            pltpu.VMEM((N_GROUPS, 2, 2, ROWS_L1 // 2, wide), bf16),
            pltpu.VMEM((N_GROUPS, 2, 2, ROWS_L1, wide), bf16),
            pltpu.VMEM((N_GROUPS, 2, 2, ROWS_L2 // 2, wide), bf16),
            pltpu.VMEM((N_GROUPS, 2, 2, ROWS_L2, wide), bf16),
            pltpu.VMEM((N_GROUPS, 2, ROWS_L2, wide), bf16),
            pltpu.SemaphoreType.DMA((N_GROUPS, 2, 16)),
            pltpu.SemaphoreType.DMA((N_GROUPS, 2, 16)),
            pltpu.SemaphoreType.DMA((16, 2)),
            pltpu.SemaphoreType.DMA((16, 2)),
            pltpu.SemaphoreType.DMA((4 + len(acts),)),
            pltpu.SemaphoreType.DMA((N_GROUPS, 4)),
            pltpu.SemaphoreType.DMA((N_GROUPS, 2)),
        ],
        compiler_params=pltpu.CompilerParams(collective_id=0, has_side_effects=True, vmem_limit_bytes=62 * 1024 * 1024),
        cost_estimate=pl.CostEstimate(
            flops=2 * seq_len * depth * rows.shape[1], bytes_accessed=2 * (seq_len * depth + 8 * depth * wide + 2 * rows.size), transcendentals=0),
    )(*acts, w_out, w_down, rows)


def solution(mesh):
    row_spec = P(("dp", "fsdp"), None, None)

    def local_layer(hidden, positions, norm_gain, w_query, w_key, w_value, w_gate, w_up, w_out, w_down):
        rows = hidden[0]
        cos_t, sin_t = rope_tables(positions, w_key.shape[1])
        acts = first_products(rows, norm_gain, w_query, w_key, w_value, w_gate, w_up, cos_t, sin_t)
        return second_product(acts, w_out, w_down, rows)[None]

    in_specs = (row_spec, P(None), P("fsdp"), P("fsdp", "tp"), P("fsdp", None), P("fsdp", None), P("fsdp", "tp"), P("fsdp", "tp"), P("tp", "fsdp"), P("tp", "fsdp"))
    return jax.shard_map(local_layer, mesh=mesh, in_specs=in_specs, out_specs=row_spec, check_vma=False)
```

```python
import functools

import jax
import jax.numpy as jnp
import numpy as np
from jax import lax
from jax.experimental import pallas as pl
from jax.experimental.pallas import tpu as pltpu
from jax.sharding import PartitionSpec as P

MESH = pl.DeviceIdType.MESH
NORM_EPS = 1e-6


def rope_tables(positions, head_dim):
    inv_freq = 10000.0 ** (-jnp.arange(0, head_dim, 2, dtype=jnp.float32) / head_dim)
    angles = positions.astype(jnp.float32)[:, None] * inv_freq[None, :]
    angles = jnp.concatenate([angles, angles], axis=-1)
    return jnp.cos(angles), jnp.sin(angles)


FF_TILE = 256


def first_kernel(
    rows_hbm, gain_hbm, wq_hbm, wk_hbm, wv_hbm, wg_hbm, wu_hbm, cos_ref, sin_ref, pick_ref, pick_rot_ref, place_ref,
    attn_hbm, z_hbm,
    act, gains, wq, wk, wv, wff, q_heads, k_rot, values, zbuf,
    send_sem, recv_sem, gain_send, gain_recv, load_sem, act_sem, out_sem,
):
    n = 8
    fs = lax.axis_index("fsdp")
    core = lax.rem(fs, 2)
    chip = lax.div(fs, 2)
    depth = wq_hbm.shape[0]
    half = depth // 2
    seq_len = rows_hbm.shape[0]
    n_chunks = wg_hbm.shape[1] // FF_TILE

    def device(by_chip, other):
        c = core if not other else 1 - core
        return lax.rem(chip + by_chip + 4, 4) * 2 + c

    right, left, sib = ({"fsdp": device(*p)} for p in ((1, 0), (-1, 0), (0, 1)))
    places = [(0, 0), (0, 1), (-1, 0), (-1, 1), (1, 0), (1, 1), (2, 0), (2, 1)]

    barrier = pltpu.get_barrier_semaphore()
    for by in range(1, n):
        pl.semaphore_signal(barrier, inc=1, device_id={"fsdp": lax.rem(fs + by, n)}, device_id_type=MESH)
    pl.semaphore_wait(barrier, n - 1)

    def qkv_streams():
        return [(0, wq_hbm, lambda at: wq.at[at, :]), (1, wk_hbm, lambda at: wk.at[:, at]), (2, wv_hbm, lambda at: wv.at[:, at])]

    def ff_streams(c):
        cols = pl.ds(pl.multiple_of(c * FF_TILE, FF_TILE), FF_TILE)
        return [
            (3 + 2 * c, wg_hbm.at[:, cols], lambda at: wff.at[c, at, pl.ds(0, FF_TILE)]),
            (4 + 2 * c, wu_hbm.at[:, cols], lambda at: wff.at[c, at, pl.ds(FF_TILE, FF_TILE)]),
        ]

    messages = [
        (2 * depth, depth, None, right), (4 * depth, depth, None, left),
        (6 * depth, half, 2 * depth, right), (6 * depth + half, half, 4 * depth + half, left),
        (depth, depth, None, sib), (3 * depth, depth, 2 * depth, sib), (5 * depth, depth, 4 * depth, sib),
        (7 * depth, half, 6 * depth, sib), (7 * depth + half, half, 6 * depth + half, sib),
    ]

    def message(stream, idx):
        row, own, gathered = stream
        dst, size, src, peer = messages[idx]
        return pltpu.make_async_remote_copy(
            src_ref=own if src is None else gathered(pl.ds(src, size)), dst_ref=gathered(pl.ds(dst, size)),
            send_sem=send_sem.at[row, idx], recv_sem=recv_sem.at[row, idx], device_id=peer, device_id_type=MESH)

    def own_load(stream):
        row, own, gathered = stream
        return pltpu.make_async_copy(own, gathered(pl.ds(0, depth)), load_sem.at[row])

    def send(streams, *idxs):
        for idx in idxs:
            for stream in streams:
                message(stream, idx).start()

    def receive(streams, *idxs):
        for idx in idxs:
            for stream in streams:
                message(stream, idx).wait_recv()

    def begin(streams):
        send(streams, 0, 1, 4)
        for stream in streams:
            own_load(stream).start()

    def pass_on(streams):
        receive(streams, 0, 1)
        send(streams, 2, 3, 5, 6)

    def complete(streams):
        receive(streams, 2, 3)
        send(streams, 7, 8)
        for stream in streams:
            own_load(stream).wait()
        receive(streams, 4, 5, 6, 7, 8)

    def gain_copy(slot):
        by_chip, other = places[slot]
        return pltpu.make_async_remote_copy(
            src_ref=gain_hbm, dst_ref=gains.at[slot], send_sem=gain_send.at[slot], recv_sem=gain_recv.at[slot],
            device_id={"fsdp": device(-by_chip, other)}, device_id_type=MESH)

    for slot in range(1, n):
        gain_copy(slot).start()
    begin(qkv_streams())
    begin(ff_streams(0))
    own_gain = pltpu.make_async_copy(gain_hbm, gains.at[0], gain_send.at[0])
    own_gain.start()
    blocks = []
    for slot, place in enumerate(places):
        cols = pl.ds(pl.multiple_of(device(*place) * depth, 128), depth)
        blocks.append(pltpu.make_async_copy(rows_hbm.at[:, cols], act.at[:, pl.ds(slot * depth, depth)], act_sem.at[slot]))
    for block in blocks:
        block.start()
    own_gain.wait()
    for slot in range(1, n):
        gain_copy(slot).wait()
    for block in blocks:
        block.wait()

    @pl.loop(0, seq_len // 16)
    def _(r):
        where = pl.ds(pl.multiple_of(r * 16, 16), 16)
        row_f32 = act[where, :].astype(jnp.float32)
        centered = row_f32 - jnp.mean(row_f32, axis=-1, keepdims=True)
        variance = jnp.mean(centered * centered, axis=-1, keepdims=True)
        scaled = centered * lax.rsqrt(variance + NORM_EPS)
        for slot in range(n):
            cols = slice(slot * depth, (slot + 1) * depth)
            act[where, cols] = (scaled[:, cols] * gains[slot]).astype(jnp.bfloat16)

    pass_on(qkv_streams())
    begin(ff_streams(1))
    pass_on(ff_streams(0))
    begin(ff_streams(2))
    complete(qkv_streams())

    n_heads, _, head_dim = pick_ref.shape

    def dot_t(a, b):
        return lax.dot_general(a, b, (((1,), (1,)), ((), ())), preferred_element_type=jnp.float32)

    q_block = 256

    @pl.loop(0, seq_len // q_block)
    def _(m):
        where = pl.ds(pl.multiple_of(m * q_block, q_block), q_block)
        cos_t, sin_t = cos_ref[where, :], sin_ref[where, :]
        dot = functools.partial(jnp.dot, preferred_element_type=jnp.float32)
        query_raw = dot(act[where, :], wq[...]).astype(jnp.bfloat16)
        for h in range(n_heads):
            rotated = dot(query_raw, pick_ref[h]) * cos_t + dot(query_raw, pick_rot_ref[h]) * sin_t
            q_heads[h, where, :] = rotated.astype(jnp.bfloat16)
        key_raw = dot_t(act[where, :], wk[...]).astype(jnp.bfloat16)
        key_turned = dot(key_raw, pick_rot_ref[0, 0:head_dim, :])
        k_rot[where, :] = (key_raw.astype(jnp.float32) * cos_t + key_turned * sin_t).astype(jnp.bfloat16)
        values[where, :] = dot_t(act[where, :], wv[...]).astype(jnp.bfloat16)

    for idx in range(9):
        message(qkv_streams()[0], idx).wait_send()
    pass_on(ff_streams(1))
    begin(ff_streams(3))

    score_scale = head_dim ** -0.5
    for blk in range(seq_len // q_block):
        lo, hi = blk * q_block, (blk + 1) * q_block
        causal_mask = lax.broadcasted_iota(jnp.int32, (q_block, hi), 1) <= lo + lax.broadcasted_iota(jnp.int32, (q_block, hi), 0)
        wq[lo:hi, :] = jnp.zeros((q_block, wq.shape[1]), jnp.bfloat16)

        @pl.loop(0, n_heads)
        def _(h):
            scores = dot_t(q_heads[h, lo:hi, :], k_rot[0:hi, :]) * score_scale
            scores = jnp.where(causal_mask, scores, -1e30)
            weights = jnp.exp(scores - jnp.max(scores, axis=-1, keepdims=True))
            prob_rows = (weights / jnp.sum(weights, axis=-1, keepdims=True)).astype(jnp.bfloat16)
            out = jnp.dot(prob_rows, values[0:hi, :], preferred_element_type=jnp.float32).astype(jnp.bfloat16)
            placed = jnp.dot(out, place_ref[h], preferred_element_type=jnp.float32).astype(jnp.bfloat16)
            wq[lo:hi, :] = wq[lo:hi, :] + placed

    attn_out = pltpu.make_async_copy(wq.at[pl.ds(0, seq_len), :], attn_hbm, out_sem.at[n_chunks])
    attn_out.start()

    def z_out(c):
        cols = pl.ds(pl.multiple_of(c * FF_TILE, FF_TILE), FF_TILE)
        return pltpu.make_async_copy(zbuf.at[lax.rem(c, 2)], z_hbm.at[:, cols], out_sem.at[c])

    @pl.loop(0, n_chunks)
    def _(c):
        @pl.when(c + 2 < n_chunks)
        def _():
            pass_on(ff_streams(c + 2))

        @pl.when(c + 4 < n_chunks)
        def _():
            begin(ff_streams(c + 4))

        complete(ff_streams(c))

        @pl.when(c >= 2)
        def _():
            z_out(c - 2).wait()

        @pl.loop(0, seq_len // 256)
        def _(m):
            where = pl.ds(pl.multiple_of(m * 256, 256), 256)
            both = jnp.dot(act[where, :], wff[c], preferred_element_type=jnp.float32)
            gate = both[:, :FF_TILE].astype(jnp.bfloat16).astype(jnp.float32)
            up = both[:, FF_TILE:].astype(jnp.bfloat16).astype(jnp.float32)
            zbuf[lax.rem(c, 2), where, :] = (gate * jax.nn.sigmoid(gate) * up).astype(jnp.bfloat16)

        z_out(c).start()

    for c in (n_chunks - 2, n_chunks - 1):
        z_out(c).wait()
    attn_out.wait()
    for stream in qkv_streams()[1:]:
        for idx in range(9):
            message(stream, idx).wait_send()

    @pl.loop(0, n_chunks)
    def _(c):
        for stream in ff_streams(c):
            for idx in range(9):
                message(stream, idx).wait_send()


def first_products(rows, norm_gain, w_query, w_key, w_value, w_gate, w_up, cos_t, sin_t):
    seq_len, width = rows.shape
    q_width, head_dim, ff = w_query.shape[1], w_key.shape[1], w_gate.shape[1]
    n_heads = q_width // head_dim
    n_chunks = ff // FF_TILE
    bf16 = jnp.bfloat16
    feature = np.arange(head_dim)
    head = np.arange(n_heads)[:, None, None] * head_dim
    source = np.arange(q_width)[None, :, None]
    one_hot = np.where(source == head + feature, 1.0, 0.0)
    turned = np.where(feature < head_dim // 2, feature + head_dim // 2, feature - head_dim // 2)
    sign = np.where(feature < head_dim // 2, -1.0, 1.0)
    pick = jnp.asarray(one_hot, bf16)
    pick_rot = jnp.asarray(np.where(source == head + turned, sign, 0.0), bf16)
    place = jnp.asarray(one_hot.transpose(0, 2, 1), bf16)
    hbm = pl.BlockSpec(memory_space=pl.ANY)
    vmem = pl.BlockSpec(memory_space=pltpu.VMEM)
    return pl.pallas_call(
        first_kernel,
        in_specs=[hbm] * 7 + [vmem] * 5,
        out_specs=[hbm, hbm],
        out_shape=[jax.ShapeDtypeStruct((seq_len, q_width), bf16), jax.ShapeDtypeStruct((seq_len, ff), bf16)],
        scratch_shapes=[
            pltpu.VMEM((seq_len, width), bf16),
            pltpu.VMEM((8, 1, width // 8), jnp.float32),
            pltpu.VMEM((width, q_width), bf16),
            pltpu.VMEM((head_dim, width), bf16),
            pltpu.VMEM((head_dim, width), bf16),
            pltpu.VMEM((n_chunks, width, 2 * FF_TILE), bf16),
            pltpu.VMEM((n_heads, seq_len, head_dim), bf16),
            pltpu.VMEM((seq_len, head_dim), bf16),
            pltpu.VMEM((seq_len, head_dim), bf16),
            pltpu.VMEM((2, seq_len, FF_TILE), bf16),
            pltpu.SemaphoreType.DMA((3 + 2 * n_chunks, 9)),
            pltpu.SemaphoreType.DMA((3 + 2 * n_chunks, 9)),
            pltpu.SemaphoreType.DMA((8,)),
            pltpu.SemaphoreType.DMA((8,)),
            pltpu.SemaphoreType.DMA((3 + 2 * n_chunks,)),
            pltpu.SemaphoreType.DMA((8,)),
            pltpu.SemaphoreType.DMA((n_chunks + 1,)),
        ],
        compiler_params=pltpu.CompilerParams(collective_id=1, has_side_effects=True, vmem_limit_bytes=67043328),
    )(rows, norm_gain.reshape(1, -1), w_query, w_key.T, w_value.T, w_gate, w_up, cos_t, sin_t, pick, pick_rot, place)


ROWS_L1 = 128
ROWS_L2 = 32
N_GROUPS = 8
PERIOD = 5
STAGES = 9
PART_SLOTS = 5


def reduce_kernel(n_acts, *refs):
    acts_hbm = refs[:n_acts]
    reduce_body(acts_hbm, *refs[n_acts:])


def reduce_body(
    acts_hbm, wo_hbm, wd_hbm, rows_hbm, out_hbm,
    act, weight, part, whole, recv1, recv2, recv3, recv4, resid,
    send_sem, recv_sem, xsend_sem, xrecv_sem, load_sem, resid_sem, out_sem,
):
    n_fsdp = 8
    tp = lax.axis_index("tp")
    fs = lax.axis_index("fsdp")
    coord = {"y": lax.rem(tp, 4), "z": lax.div(tp, 4)}
    core = lax.rem(fs, 2)
    full = wo_hbm.shape[1]
    cols = full // 2
    split = wo_hbm.shape[0]

    def at(axis, delta):
        moved = lax.rem(coord[axis] + delta + 4, 4)
        return {"tp": coord["z"] * 4 + moved if axis == "y" else moved * 4 + coord["y"]}

    right = {"fsdp": lax.rem(fs + 2, n_fsdp)}
    left = {"fsdp": lax.rem(fs + n_fsdp - 2, n_fsdp)}
    sib = {"fsdp": fs + 1 - 2 * core}

    def xcopy(src, slot, peer):
        return pltpu.make_async_remote_copy(
            src_ref=src, dst_ref=weight.at[slot], send_sem=xsend_sem.at[slot, 0], recv_sem=xrecv_sem.at[slot, 0],
            device_id=peer, device_id_type=MESH)

    def own_parts(half):
        where = pl.ds(half * cols, cols)
        return [(wo_hbm.at[:, where], pl.ds(0, split)), (wd_hbm.at[:, where], pl.ds(split, wd_hbm.shape[0]))]

    def own_copies(slot, peer):
        return [
            pltpu.make_async_remote_copy(
                src_ref=src, dst_ref=weight.at[slot, at], send_sem=xsend_sem.at[slot, j], recv_sem=xrecv_sem.at[slot, j],
                device_id=peer, device_id_type=MESH)
            for j, (src, at) in enumerate(own_parts(slot % 2))
        ]

    own_sends = [(4, right), (8, left), (2, sib), (5, right), (9, left), (3, sib)]
    relays = [(6, sib), (7, sib), (10, sib), (11, sib), (12, right), (13, left), (14, sib), (15, sib)]

    def x_wait_recv(slot):
        if slot in (2, 3, 4, 5, 8, 9):
            for copy in own_copies(slot, sib):
                copy.wait_recv()
        else:
            xcopy(weight.at[slot], slot, sib).wait_recv()

    loads = []
    for half in range(2):
        for j, (src, part_rows) in enumerate(own_parts(half)):
            loads.append(pltpu.make_async_copy(src, weight.at[half, part_rows], load_sem.at[2 * half + j]))
    col = 0
    for idx, act_hbm in enumerate(acts_hbm):
        size = act_hbm.shape[1]
        loads.append(pltpu.make_async_copy(act_hbm, act.at[:, pl.ds(col, size)], load_sem.at[4 + idx]))
        col += size
    for load in loads:
        load.start()

    barrier = pltpu.get_barrier_semaphore()
    peers = [at("y", 1), at("y", -1), at("z", 1), at("z", -1), right, left, sib]
    for peer in peers:
        pl.semaphore_signal(barrier, inc=1, device_id=peer, device_id_type=MESH)
    pl.semaphore_wait(barrier, len(peers))

    for slot, peer in own_sends:
        for copy in own_copies(slot, peer):
            copy.start()
    for load in loads:
        load.wait()

    halves = [("y", "z"), ("z", "y")]

    def pslot(g):
        return lax.rem(g, PART_SLOTS)

    def block1(x, delta):
        k = lax.rem(coord[halves[x][0]] + delta + 4, 4)
        return pl.multiple_of(x * 4 * ROWS_L1 + k * ROWS_L1, ROWS_L1)

    def block2(x, delta):
        k = lax.rem(coord[halves[x][1]] + delta + 4, 4)
        return pl.multiple_of(block1(x, 0) + k * ROWS_L2, ROWS_L2)

    def offset(base, add):
        return pl.multiple_of(base + add, 16)

    def message(g, x, kind, src, dst, axis, delta):
        return pltpu.make_async_remote_copy(
            src_ref=src, dst_ref=dst, send_sem=send_sem.at[g, x, kind], recv_sem=recv_sem.at[g, x, kind],
            device_id=at(axis, delta), device_id_type=MESH)

    def scatter_far(g, x, level):
        block, axis, buf, rows, kind = (block1, halves[x][0], recv1, ROWS_L1, 0) if level == 1 else (block2, halves[x][1], recv3, ROWS_L2, 4)
        half = rows // 2
        far = block(x, 2)
        return [
            message(g, x, kind, part.at[pslot(g), pl.ds(far, half), :], buf.at[g, x, 0], axis, 1),
            message(g, x, kind + 1, part.at[pslot(g), pl.ds(offset(far, half), half), :], buf.at[g, x, 1], axis, -1),
        ]

    def scatter_near(g, x, level):
        block, axis, buf, rows, kind = (block1, halves[x][0], recv2, ROWS_L1, 2) if level == 1 else (block2, halves[x][1], recv4, ROWS_L2, 6)
        return [
            message(g, x, kind, part.at[pslot(g), pl.ds(block(x, 1), rows), :], buf.at[g, x, 0], axis, 1),
            message(g, x, kind + 1, part.at[pslot(g), pl.ds(block(x, -1), rows), :], buf.at[g, x, 1], axis, -1),
        ]

    def gather_near(g, x, level):
        block, axis, rows, kind = (block1, halves[x][0], ROWS_L1, 12) if level == 1 else (block2, halves[x][1], ROWS_L2, 8)
        mine = whole.at[g, pl.ds(block(x, 0), rows), :]
        return [message(g, x, kind, mine, mine, axis, 1), message(g, x, kind + 1, mine, mine, axis, -1)]

    def gather_far(g, x, level):
        block, axis, rows, kind = (block1, halves[x][0], ROWS_L1, 14) if level == 1 else (block2, halves[x][1], ROWS_L2, 10)
        half = rows // 2
        lo = whole.at[g, pl.ds(block(x, -1), half), :]
        hi = whole.at[g, pl.ds(offset(block(x, 1), half), half), :]
        return [message(g, x, kind, lo, lo, axis, 1), message(g, x, kind + 1, hi, hi, axis, -1)]

    def start(copies):
        for copy in copies:
            copy.start()

    def finish(copies):
        for copy in copies:
            copy.wait()

    def summed(g, row, rows, *refs):
        total = part[pslot(g), pl.ds(row, rows), :].astype(jnp.float32)
        for ref in refs:
            total = total + ref.astype(jnp.float32)
        return total.astype(jnp.bfloat16)

    def add_into(g, row, rows, *refs):
        part[pslot(g), pl.ds(row, rows), :] = summed(g, row, rows, *refs)

    def group_info(g):
        mid = jnp.logical_and(g >= 2, g < 6)
        i = g - 2
        odd = lax.rem(i + 2, 2)
        slot = jnp.where(g < 2, g, jnp.where(mid, 4 + 4 * odd + lax.div(i + 2, 2) - 1, g + 6))
        delta = jnp.where(g < 2, 0, jnp.where(mid, 2 * odd - 1, 2))
        half = jnp.where(mid, lax.div(i + 2, 2) - 1, lax.rem(g, 2))
        chip = lax.rem(lax.div(fs, 2) + delta + 4, 4)
        col_a = pl.multiple_of((chip * 2 + core) * full + half * cols, 128)
        col_b = pl.multiple_of((chip * 2 + 1 - core) * full + half * cols, 128)
        return slot, col_a, col_b

    def resid_copies(g):
        _, col_a, col_b = group_info(g)
        copies = []
        for x in range(2):
            for j, col in enumerate((col_a, col_b)):
                copies.append(pltpu.make_async_copy(
                    rows_hbm.at[pl.ds(block2(x, 0), ROWS_L2), pl.ds(col, cols)],
                    resid.at[g, x, :, pl.ds(j * cols, cols)], resid_sem.at[g, 2 * x + j]))
        return copies

    def out_copies(g):
        _, col_a, col_b = group_info(g)
        return [
            pltpu.make_async_copy(whole.at[g, :, pl.ds(j * cols, cols)], out_hbm.at[:, pl.ds(col, cols)], out_sem.at[g, j])
            for j, col in enumerate((col_a, col_b))
        ]

    def stage0(g):
        slot, _, _ = group_info(g)
        start(resid_copies(g))

        @pl.when(g == 2)
        def _():
            x_wait_recv(4)
            xcopy(weight.at[4], 6, sib).start()
            xcopy(weight.at[4], 12, right).start()
            x_wait_recv(8)
            xcopy(weight.at[8], 10, sib).start()

        @pl.when(g == 4)
        def _():
            x_wait_recv(5)
            xcopy(weight.at[5], 7, sib).start()
            x_wait_recv(9)
            xcopy(weight.at[9], 11, sib).start()
            xcopy(weight.at[9], 13, left).start()

        @pl.when(g == 6)
        def _():
            x_wait_recv(12)
            xcopy(weight.at[12], 14, sib).start()
            x_wait_recv(13)
            xcopy(weight.at[13], 15, sib).start()

        for known, known_slot in enumerate((2, 3, 6, 10, 7, 11, 14, 15)):
            @pl.when(g == known)
            def _():
                x_wait_recv(known_slot)

        @pl.loop(0, act.shape[0] // 256)
        def _(m):
            where = pl.ds(pl.multiple_of(m * 256, 256), 256)
            for j in range(2):
                value = jnp.dot(act[where, :], weight[slot + 2 * j], preferred_element_type=jnp.float32)
                part[pslot(g), where, j * cols : (j + 1) * cols] = value.astype(jnp.bfloat16)

        for x in range(2):
            start(scatter_far(g, x, 1))

    def scatter_mid(level):
        def run(g):
            buf = recv1 if level == 1 else recv3
            rows = ROWS_L1 if level == 1 else ROWS_L2
            block = block1 if level == 1 else block2
            for x in range(2):
                finish(scatter_far(g, x, level))
                add_into(g, block(x, 1), rows // 2, buf[g, x, 0])
                add_into(g, offset(block(x, -1), rows // 2), rows // 2, buf[g, x, 1])
            for x in range(2):
                start(scatter_near(g, x, level))
        return run

    def stage2(g):
        for x in range(2):
            finish(scatter_near(g, x, 1))
            add_into(g, block1(x, 0), ROWS_L1, recv2[g, x, 0], recv2[g, x, 1])
        for x in range(2):
            start(scatter_far(g, x, 2))

    def stage4(g):
        finish(resid_copies(g))
        for x in range(2):
            finish(scatter_near(g, x, 2))
            whole[g, pl.ds(block2(x, 0), ROWS_L2), :] = summed(g, block2(x, 0), ROWS_L2, recv4[g, x, 0], recv4[g, x, 1], resid[g, x])
        for x in range(2):
            start(gather_near(g, x, 2))

    def relay(done, then):
        def run(g):
            for x in range(2):
                finish(done[0](g, x, done[1]))
                start(then[0](g, x, then[1]))
        return run

    def stage8(g):
        for x in range(2):
            finish(gather_far(g, x, 1))
        start(out_copies(g))

    stages = [
        stage0, scatter_mid(1), stage2, scatter_mid(2), stage4,
        relay((gather_near, 2), (gather_far, 2)), relay((gather_far, 2), (gather_near, 1)),
        relay((gather_near, 1), (gather_far, 1)), stage8,
    ]

    @pl.loop(0, (N_GROUPS // 2 - 1) * PERIOD + 1 + STAGES)
    def _(t):
        for s in reversed(range(STAGES)):
            d = t - s
            pair, second = lax.div(d + 2 * PERIOD, PERIOD) - 2, lax.rem(d + 2 * PERIOD, PERIOD)
            g = 2 * pair + second
            inside = jnp.logical_and(d >= 0, d < (N_GROUPS // 2) * PERIOD)

            @pl.when(jnp.logical_and(inside, second < 2))
            def _():
                stages[s](g)

    @pl.loop(0, N_GROUPS)
    def _(g):
        finish(out_copies(g))

    for slot, peer in own_sends:
        for copy in own_copies(slot, peer):
            copy.wait_send()
    for slot, peer in relays:
        xcopy(weight.at[slot], slot, peer).wait_send()


def second_product(acts, w_out, w_down, rows):
    seq_len = rows.shape[0]
    depth = w_out.shape[0] + w_down.shape[0]
    wide = w_out.shape[1]
    cols = wide // 2
    bf16 = jnp.bfloat16
    return pl.pallas_call(
        functools.partial(reduce_kernel, len(acts)),
        in_specs=[pl.BlockSpec(memory_space=pl.ANY)] * (len(acts) + 3),
        out_specs=pl.BlockSpec(memory_space=pl.ANY),
        out_shape=jax.ShapeDtypeStruct(rows.shape, bf16),
        scratch_shapes=[
            pltpu.VMEM((seq_len, depth), bf16),
            pltpu.VMEM((16, depth, cols), bf16),
            pltpu.VMEM((PART_SLOTS, seq_len, wide), bf16),
            pltpu.VMEM((N_GROUPS, seq_len, wide), bf16),
            pltpu.VMEM((N_GROUPS, 2, 2, ROWS_L1 // 2, wide), bf16),
            pltpu.VMEM((N_GROUPS, 2, 2, ROWS_L1, wide), bf16),
            pltpu.VMEM((N_GROUPS, 2, 2, ROWS_L2 // 2, wide), bf16),
            pltpu.VMEM((N_GROUPS, 2, 2, ROWS_L2, wide), bf16),
            pltpu.VMEM((N_GROUPS, 2, ROWS_L2, wide), bf16),
            pltpu.SemaphoreType.DMA((N_GROUPS, 2, 16)),
            pltpu.SemaphoreType.DMA((N_GROUPS, 2, 16)),
            pltpu.SemaphoreType.DMA((16, 2)),
            pltpu.SemaphoreType.DMA((16, 2)),
            pltpu.SemaphoreType.DMA((4 + len(acts),)),
            pltpu.SemaphoreType.DMA((N_GROUPS, 4)),
            pltpu.SemaphoreType.DMA((N_GROUPS, 2)),
        ],
        compiler_params=pltpu.CompilerParams(collective_id=0, has_side_effects=True, vmem_limit_bytes=62 * 1024 * 1024),
        cost_estimate=pl.CostEstimate(
            flops=2 * seq_len * depth * rows.shape[1], bytes_accessed=2 * (seq_len * depth + 8 * depth * wide + 2 * rows.size), transcendentals=0),
    )(*acts, w_out, w_down, rows)


def solution(mesh):
    row_spec = P(("dp", "fsdp"), None, None)

    def local_layer(hidden, positions, norm_gain, w_query, w_key, w_value, w_gate, w_up, w_out, w_down):
        rows = hidden[0]
        cos_t, sin_t = rope_tables(positions, w_key.shape[1])
        acts = first_products(rows, norm_gain, w_query, w_key, w_value, w_gate, w_up, cos_t, sin_t)
        return second_product(acts, w_out, w_down, rows)[None]

    in_specs = (row_spec, P(None), P("fsdp"), P("fsdp", "tp"), P("fsdp", None), P("fsdp", None), P("fsdp", "tp"), P("fsdp", "tp"), P("tp", "fsdp"), P("tp", "fsdp"))
    return jax.shard_map(local_layer, mesh=mesh, in_specs=in_specs, out_specs=row_spec, check_vma=False)
```

```python
import functools

import jax
import jax.numpy as jnp
import numpy as np
from jax import lax
from jax.experimental import pallas as pl
from jax.experimental.pallas import tpu as pltpu
from jax.sharding import PartitionSpec as P

MESH = pl.DeviceIdType.MESH
NORM_EPS = 1e-6


def rope_tables(positions, head_dim):
    inv_freq = 10000.0 ** (-jnp.arange(0, head_dim, 2, dtype=jnp.float32) / head_dim)
    angles = positions.astype(jnp.float32)[:, None] * inv_freq[None, :]
    angles = jnp.concatenate([angles, angles], axis=-1)
    return jnp.cos(angles), jnp.sin(angles)


FF_TILE = 256


def first_kernel(
    rows_hbm, gain_hbm, wq_hbm, wk_hbm, wv_hbm, wg_hbm, wu_hbm, wo_hbm, cos_ref, sin_ref, pick_ref, pick_rot_ref, place_ref,
    attn_hbm, z_hbm, pre_hbm,
    act, gains, wq, wk, wv, wff, q_heads, k_rot, values, zbuf,
    send_sem, recv_sem, gain_send, gain_recv, load_sem, act_sem, out_sem, pre_send, pre_recv,
):
    n = 8
    fs = lax.axis_index("fsdp")
    core = lax.rem(fs, 2)
    chip = lax.div(fs, 2)
    depth = wq_hbm.shape[0]
    half = depth // 2
    seq_len = rows_hbm.shape[0]
    n_chunks = wg_hbm.shape[1] // FF_TILE

    def device(by_chip, other):
        c = core if not other else 1 - core
        return lax.rem(chip + by_chip + 4, 4) * 2 + c

    right, left, sib = ({"fsdp": device(*p)} for p in ((1, 0), (-1, 0), (0, 1)))
    places = [(0, 0), (0, 1), (-1, 0), (-1, 1), (1, 0), (1, 1), (2, 0), (2, 1)]

    barrier = pltpu.get_barrier_semaphore()
    for by in range(1, n):
        pl.semaphore_signal(barrier, inc=1, device_id={"fsdp": lax.rem(fs + by, n)}, device_id_type=MESH)
    pl.semaphore_wait(barrier, n - 1)

    def qkv_streams():
        return [(0, wq_hbm, lambda at: wq.at[at, :]), (1, wk_hbm, lambda at: wk.at[:, at]), (2, wv_hbm, lambda at: wv.at[:, at])]

    def ff_streams(c):
        cols = pl.ds(pl.multiple_of(c * FF_TILE, FF_TILE), FF_TILE)
        return [
            (3 + 2 * c, wg_hbm.at[:, cols], lambda at: wff.at[c, at, pl.ds(0, FF_TILE)]),
            (4 + 2 * c, wu_hbm.at[:, cols], lambda at: wff.at[c, at, pl.ds(FF_TILE, FF_TILE)]),
        ]

    messages = [
        (2 * depth, depth, None, right), (4 * depth, depth, None, left),
        (6 * depth, half, 2 * depth, right), (6 * depth + half, half, 4 * depth + half, left),
        (depth, depth, None, sib), (3 * depth, depth, 2 * depth, sib), (5 * depth, depth, 4 * depth, sib),
        (7 * depth, half, 6 * depth, sib), (7 * depth + half, half, 6 * depth + half, sib),
    ]

    def message(stream, idx):
        row, own, gathered = stream
        dst, size, src, peer = messages[idx]
        return pltpu.make_async_remote_copy(
            src_ref=own if src is None else gathered(pl.ds(src, size)), dst_ref=gathered(pl.ds(dst, size)),
            send_sem=send_sem.at[row, idx], recv_sem=recv_sem.at[row, idx], device_id=peer, device_id_type=MESH)

    def own_load(stream):
        row, own, gathered = stream
        return pltpu.make_async_copy(own, gathered(pl.ds(0, depth)), load_sem.at[row])

    def send(streams, *idxs):
        for idx in idxs:
            for stream in streams:
                message(stream, idx).start()

    def receive(streams, *idxs):
        for idx in idxs:
            for stream in streams:
                message(stream, idx).wait_recv()

    def begin(streams):
        send(streams, 0, 1, 4)
        for stream in streams:
            own_load(stream).start()

    def pass_on(streams):
        receive(streams, 0, 1)
        send(streams, 2, 3, 5, 6)

    def complete(streams):
        receive(streams, 2, 3)
        send(streams, 7, 8)
        for stream in streams:
            own_load(stream).wait()
        receive(streams, 4, 5, 6, 7, 8)

    def gain_copy(slot):
        by_chip, other = places[slot]
        return pltpu.make_async_remote_copy(
            src_ref=gain_hbm, dst_ref=gains.at[slot], send_sem=gain_send.at[slot], recv_sem=gain_recv.at[slot],
            device_id={"fsdp": device(-by_chip, other)}, device_id_type=MESH)

    for slot in range(1, n):
        gain_copy(slot).start()
    begin(qkv_streams())
    begin(ff_streams(0))
    own_gain = pltpu.make_async_copy(gain_hbm, gains.at[0], gain_send.at[0])
    own_gain.start()
    blocks = []
    for slot, place in enumerate(places):
        cols = pl.ds(pl.multiple_of(device(*place) * depth, 128), depth)
        blocks.append(pltpu.make_async_copy(rows_hbm.at[:, cols], act.at[:, pl.ds(slot * depth, depth)], act_sem.at[slot]))
    for block in blocks:
        block.start()
    own_gain.wait()
    for slot in range(1, n):
        gain_copy(slot).wait()
    for block in blocks:
        block.wait()

    @pl.loop(0, seq_len // 16)
    def _(r):
        where = pl.ds(pl.multiple_of(r * 16, 16), 16)
        row_f32 = act[where, :].astype(jnp.float32)
        centered = row_f32 - jnp.mean(row_f32, axis=-1, keepdims=True)
        variance = jnp.mean(centered * centered, axis=-1, keepdims=True)
        scaled = centered * lax.rsqrt(variance + NORM_EPS)
        for slot in range(n):
            cols = slice(slot * depth, (slot + 1) * depth)
            act[where, cols] = (scaled[:, cols] * gains[slot]).astype(jnp.bfloat16)

    pass_on(qkv_streams())
    begin(ff_streams(1))
    pass_on(ff_streams(0))
    begin(ff_streams(2))
    complete(qkv_streams())

    n_heads, _, head_dim = pick_ref.shape

    def dot_t(a, b):
        return lax.dot_general(a, b, (((1,), (1,)), ((), ())), preferred_element_type=jnp.float32)

    q_block = 256

    @pl.loop(0, seq_len // q_block)
    def _(m):
        where = pl.ds(pl.multiple_of(m * q_block, q_block), q_block)
        cos_t, sin_t = cos_ref[where, :], sin_ref[where, :]
        dot = functools.partial(jnp.dot, preferred_element_type=jnp.float32)
        query_raw = dot(act[where, :], wq[...]).astype(jnp.bfloat16)
        for h in range(n_heads):
            rotated = dot(query_raw, pick_ref[h]) * cos_t + dot(query_raw, pick_rot_ref[h]) * sin_t
            q_heads[h, where, :] = rotated.astype(jnp.bfloat16)
        key_raw = dot_t(act[where, :], wk[...]).astype(jnp.bfloat16)
        key_turned = dot(key_raw, pick_rot_ref[0, 0:head_dim, :])
        k_rot[where, :] = (key_raw.astype(jnp.float32) * cos_t + key_turned * sin_t).astype(jnp.bfloat16)
        values[where, :] = dot_t(act[where, :], wv[...]).astype(jnp.bfloat16)

    for idx in range(9):
        message(qkv_streams()[0], idx).wait_send()
    pass_on(ff_streams(1))
    begin(ff_streams(3))

    score_scale = head_dim ** -0.5
    for blk in range(seq_len // q_block):
        lo, hi = blk * q_block, (blk + 1) * q_block
        causal_mask = lax.broadcasted_iota(jnp.int32, (q_block, hi), 1) <= lo + lax.broadcasted_iota(jnp.int32, (q_block, hi), 0)
        wq[lo:hi, :] = jnp.zeros((q_block, wq.shape[1]), jnp.bfloat16)

        @pl.loop(0, n_heads)
        def _(h):
            scores = dot_t(q_heads[h, lo:hi, :], k_rot[0:hi, :]) * score_scale
            scores = jnp.where(causal_mask, scores, -1e30)
            weights = jnp.exp(scores - jnp.max(scores, axis=-1, keepdims=True))
            prob_rows = (weights / jnp.sum(weights, axis=-1, keepdims=True)).astype(jnp.bfloat16)
            out = jnp.dot(prob_rows, values[0:hi, :], preferred_element_type=jnp.float32).astype(jnp.bfloat16)
            placed = jnp.dot(out, place_ref[h], preferred_element_type=jnp.float32).astype(jnp.bfloat16)
            wq[lo:hi, :] = wq[lo:hi, :] + placed

    attn_out = pltpu.make_async_copy(wq.at[pl.ds(0, seq_len), :], attn_hbm, out_sem.at[n_chunks])
    attn_out.start()

    def w_out_copy(side):
        return pltpu.make_async_remote_copy(
            src_ref=wo_hbm, dst_ref=pre_hbm.at[side], send_sem=pre_send.at[side], recv_sem=pre_recv.at[side],
            device_id=(right, left)[side], device_id_type=MESH)

    def z_out(c):
        cols = pl.ds(pl.multiple_of(c * FF_TILE, FF_TILE), FF_TILE)
        return pltpu.make_async_copy(zbuf.at[lax.rem(c, 2)], z_hbm.at[:, cols], out_sem.at[c])

    @pl.loop(0, n_chunks)
    def _(c):
        @pl.when(c + 2 < n_chunks)
        def _():
            pass_on(ff_streams(c + 2))

        @pl.when(c + 2 == n_chunks - 1)
        def _():
            for side in range(2):
                w_out_copy(side).start()

        @pl.when(c + 4 < n_chunks)
        def _():
            begin(ff_streams(c + 4))

        complete(ff_streams(c))

        @pl.when(c >= 2)
        def _():
            z_out(c - 2).wait()

        @pl.loop(0, seq_len // 256)
        def _(m):
            where = pl.ds(pl.multiple_of(m * 256, 256), 256)
            both = jnp.dot(act[where, :], wff[c], preferred_element_type=jnp.float32)
            gate = both[:, :FF_TILE].astype(jnp.bfloat16).astype(jnp.float32)
            up = both[:, FF_TILE:].astype(jnp.bfloat16).astype(jnp.float32)
            zbuf[lax.rem(c, 2), where, :] = (gate * jax.nn.sigmoid(gate) * up).astype(jnp.bfloat16)

        z_out(c).start()

    for c in (n_chunks - 2, n_chunks - 1):
        z_out(c).wait()
    attn_out.wait()
    for side in range(2):
        w_out_copy(side).wait()
    for stream in qkv_streams()[1:]:
        for idx in range(9):
            message(stream, idx).wait_send()

    @pl.loop(0, n_chunks)
    def _(c):
        for stream in ff_streams(c):
            for idx in range(9):
                message(stream, idx).wait_send()


def first_products(rows, norm_gain, w_query, w_key, w_value, w_gate, w_up, w_out, cos_t, sin_t):
    seq_len, width = rows.shape
    q_width, head_dim, ff = w_query.shape[1], w_key.shape[1], w_gate.shape[1]
    n_heads = q_width // head_dim
    n_chunks = ff // FF_TILE
    bf16 = jnp.bfloat16
    feature = np.arange(head_dim)
    head = np.arange(n_heads)[:, None, None] * head_dim
    source = np.arange(q_width)[None, :, None]
    one_hot = np.where(source == head + feature, 1.0, 0.0)
    turned = np.where(feature < head_dim // 2, feature + head_dim // 2, feature - head_dim // 2)
    sign = np.where(feature < head_dim // 2, -1.0, 1.0)
    pick = jnp.asarray(one_hot, bf16)
    pick_rot = jnp.asarray(np.where(source == head + turned, sign, 0.0), bf16)
    place = jnp.asarray(one_hot.transpose(0, 2, 1), bf16)
    hbm = pl.BlockSpec(memory_space=pl.ANY)
    vmem = pl.BlockSpec(memory_space=pltpu.VMEM)
    return pl.pallas_call(
        first_kernel,
        in_specs=[hbm] * 8 + [vmem] * 5,
        out_specs=[hbm] * 3,
        out_shape=[jax.ShapeDtypeStruct((seq_len, q_width), bf16), jax.ShapeDtypeStruct((seq_len, ff), bf16), jax.ShapeDtypeStruct((2, *w_out.shape), bf16)],
        scratch_shapes=[
            pltpu.VMEM((seq_len, width), bf16),
            pltpu.VMEM((8, 1, width // 8), jnp.float32),
            pltpu.VMEM((width, q_width), bf16),
            pltpu.VMEM((head_dim, width), bf16),
            pltpu.VMEM((head_dim, width), bf16),
            pltpu.VMEM((n_chunks, width, 2 * FF_TILE), bf16),
            pltpu.VMEM((n_heads, seq_len, head_dim), bf16),
            pltpu.VMEM((seq_len, head_dim), bf16),
            pltpu.VMEM((seq_len, head_dim), bf16),
            pltpu.VMEM((2, seq_len, FF_TILE), bf16),
            pltpu.SemaphoreType.DMA((3 + 2 * n_chunks, 9)),
            pltpu.SemaphoreType.DMA((3 + 2 * n_chunks, 9)),
            pltpu.SemaphoreType.DMA((8,)),
            pltpu.SemaphoreType.DMA((8,)),
            pltpu.SemaphoreType.DMA((3 + 2 * n_chunks,)),
            pltpu.SemaphoreType.DMA((8,)),
            pltpu.SemaphoreType.DMA((n_chunks + 1,)),
            pltpu.SemaphoreType.DMA((2,)),
            pltpu.SemaphoreType.DMA((2,)),
        ],
        compiler_params=pltpu.CompilerParams(collective_id=1, has_side_effects=True, vmem_limit_bytes=67043328),
    )(rows, norm_gain.reshape(1, -1), w_query, w_key.T, w_value.T, w_gate, w_up, w_out, cos_t, sin_t, pick, pick_rot, place)


ROWS_L1 = 128
ROWS_L2 = 32
N_GROUPS = 8
PERIOD = 3
STAGES = 9
PART_SLOTS = 6


def reduce_kernel(n_acts, *refs):
    acts_hbm = refs[:n_acts]
    reduce_body(acts_hbm, *refs[n_acts:])


def reduce_body(
    acts_hbm, pre_hbm, wo_hbm, wd_hbm, rows_hbm, out_hbm,
    act, weight, part, whole, recv1, recv2, recv3, recv4, resid,
    send_sem, recv_sem, xsend_sem, xrecv_sem, load_sem, resid_sem, out_sem,
):
    n_fsdp = 8
    tp = lax.axis_index("tp")
    fs = lax.axis_index("fsdp")
    coord = {"y": lax.rem(tp, 4), "z": lax.div(tp, 4)}
    core = lax.rem(fs, 2)
    full = wo_hbm.shape[1]
    cols = full // 2
    split = wo_hbm.shape[0]

    def at(axis, delta):
        moved = lax.rem(coord[axis] + delta + 4, 4)
        return {"tp": coord["z"] * 4 + moved if axis == "y" else moved * 4 + coord["y"]}

    right = {"fsdp": lax.rem(fs + 2, n_fsdp)}
    left = {"fsdp": lax.rem(fs + n_fsdp - 2, n_fsdp)}
    sib = {"fsdp": fs + 1 - 2 * core}

    def slot_ref(slot, rows=slice(None)):
        return weight.at[slot // 4 * 2 + slot % 2, rows, pl.ds(slot // 2 % 2 * cols, cols)]

    def xcopy(src, slot, peer):
        return pltpu.make_async_remote_copy(
            src_ref=src, dst_ref=slot_ref(slot), send_sem=xsend_sem.at[slot, 0], recv_sem=xrecv_sem.at[slot, 0],
            device_id=peer, device_id_type=MESH)

    def own_parts(half):
        where = pl.ds(half * cols, cols)
        return [(wo_hbm.at[:, where], pl.ds(0, split)), (wd_hbm.at[:, where], pl.ds(split, wd_hbm.shape[0]))]

    def own_copies(slot, peer):
        return [
            pltpu.make_async_remote_copy(
                src_ref=src, dst_ref=slot_ref(slot, into), send_sem=xsend_sem.at[slot, j], recv_sem=xrecv_sem.at[slot, j],
                device_id=peer, device_id_type=MESH)
            for j, (src, into) in enumerate(own_parts(slot % 2)) if j or slot in (2, 3)
        ]

    own_sends = [(4, right), (9, left), (2, sib), (5, right), (8, left), (3, sib)]
    relays = [(6, sib), (7, sib), (10, sib), (11, sib), (12, right), (13, left), (14, sib), (15, sib)]

    def x_wait_recv(slot):
        if slot in (2, 3, 4, 5, 8, 9):
            for copy in own_copies(slot, sib):
                copy.wait_recv()
        else:
            xcopy(slot_ref(slot), slot, sib).wait_recv()

    loads = []
    for half in range(2):
        for j, (src, part_rows) in enumerate(own_parts(half)):
            loads.append(pltpu.make_async_copy(src, slot_ref(half, part_rows), load_sem.at[2 * half + j]))
    for side in range(2):
        for half in range(2):
            loads.append(pltpu.make_async_copy(
                pre_hbm.at[side, :, pl.ds(half * cols, cols)], slot_ref(4 + 4 * side + half, pl.ds(0, split)), load_sem.at[4 + 2 * side + half]))
    col = 0
    for idx, act_hbm in enumerate(acts_hbm):
        size = act_hbm.shape[1]
        loads.append(pltpu.make_async_copy(act_hbm, act.at[:, pl.ds(col, size)], load_sem.at[8 + idx]))
        col += size
    for load in loads:
        load.start()

    barrier = pltpu.get_barrier_semaphore()
    peers = [at("y", 1), at("y", -1), at("z", 1), at("z", -1), right, left, sib]
    for peer in peers:
        pl.semaphore_signal(barrier, inc=1, device_id=peer, device_id_type=MESH)
    pl.semaphore_wait(barrier, len(peers))

    for slot, peer in own_sends:
        for copy in own_copies(slot, peer):
            copy.start()
    for load in loads:
        load.wait()

    halves = [("y", "z"), ("z", "y")]

    def pslot(g):
        return lax.rem(g, PART_SLOTS)

    def block1(x, delta):
        k = lax.rem(coord[halves[x][0]] + delta + 4, 4)
        return pl.multiple_of(x * 4 * ROWS_L1 + k * ROWS_L1, ROWS_L1)

    def block2(x, delta):
        k = lax.rem(coord[halves[x][1]] + delta + 4, 4)
        return pl.multiple_of(block1(x, 0) + k * ROWS_L2, ROWS_L2)

    def offset(base, add):
        return pl.multiple_of(base + add, 16)

    def message(g, x, kind, src, dst, axis, delta):
        return pltpu.make_async_remote_copy(
            src_ref=src, dst_ref=dst, send_sem=send_sem.at[g, x, kind], recv_sem=recv_sem.at[g, x, kind],
            device_id=at(axis, delta), device_id_type=MESH)

    def scatter_far(g, x, level):
        block, axis, buf, rows, kind = (block1, halves[x][0], recv1, ROWS_L1, 0) if level == 1 else (block2, halves[x][1], recv3, ROWS_L2, 4)
        half = rows // 2
        far = block(x, 2)
        return [
            message(g, x, kind, part.at[pslot(g), pl.ds(far, half), :], buf.at[g, x, 0], axis, 1),
            message(g, x, kind + 1, part.at[pslot(g), pl.ds(offset(far, half), half), :], buf.at[g, x, 1], axis, -1),
        ]

    def scatter_near(g, x, level):
        block, axis, buf, rows, kind = (block1, halves[x][0], recv2, ROWS_L1, 2) if level == 1 else (block2, halves[x][1], recv4, ROWS_L2, 6)
        return [
            message(g, x, kind, part.at[pslot(g), pl.ds(block(x, 1), rows), :], buf.at[g, x, 0], axis, 1),
            message(g, x, kind + 1, part.at[pslot(g), pl.ds(block(x, -1), rows), :], buf.at[g, x, 1], axis, -1),
        ]

    def gather_near(g, x, level):
        block, axis, rows, kind = (block1, halves[x][0], ROWS_L1, 12) if level == 1 else (block2, halves[x][1], ROWS_L2, 8)
        mine = whole.at[g, pl.ds(block(x, 0), rows), :]
        return [message(g, x, kind, mine, mine, axis, 1), message(g, x, kind + 1, mine, mine, axis, -1)]

    def gather_far(g, x, level):
        block, axis, rows, kind = (block1, halves[x][0], ROWS_L1, 14) if level == 1 else (block2, halves[x][1], ROWS_L2, 10)
        half = rows // 2
        lo = whole.at[g, pl.ds(block(x, -1), half), :]
        hi = whole.at[g, pl.ds(offset(block(x, 1), half), half), :]
        return [message(g, x, kind, lo, lo, axis, 1), message(g, x, kind + 1, hi, hi, axis, -1)]

    def start(copies):
        for copy in copies:
            copy.start()

    def finish(copies):
        for copy in copies:
            copy.wait()

    def summed(g, row, rows, *refs):
        total = part[pslot(g), pl.ds(row, rows), :].astype(jnp.float32)
        for ref in refs:
            total = total + ref.astype(jnp.float32)
        return total.astype(jnp.bfloat16)

    def add_into(g, row, rows, *refs):
        part[pslot(g), pl.ds(row, rows), :] = summed(g, row, rows, *refs)

    def group_info(g):
        mid = jnp.logical_and(g >= 2, g < 6)
        second, late = lax.rem(g, 2), lax.div(g, 4)
        half = jnp.where(mid, lax.rem(second + late, 2), second)
        slot = jnp.where(g < 2, g, jnp.where(mid, 4 + 4 * second + half, g + 6))
        delta = jnp.where(g < 2, 0, jnp.where(mid, 2 * second - 1, 2))
        chip = lax.rem(lax.div(fs, 2) + delta + 4, 4)
        col_a = pl.multiple_of((chip * 2 + core) * full + half * cols, 128)
        col_b = pl.multiple_of((chip * 2 + 1 - core) * full + half * cols, 128)
        return slot, col_a, col_b

    def resid_copies(g):
        _, col_a, col_b = group_info(g)
        copies = []
        for x in range(2):
            for j, col in enumerate((col_a, col_b)):
                copies.append(pltpu.make_async_copy(
                    rows_hbm.at[pl.ds(block2(x, 0), ROWS_L2), pl.ds(col, cols)],
                    resid.at[g, x, :, pl.ds(j * cols, cols)], resid_sem.at[g, 2 * x + j]))
        return copies

    def out_copies(g):
        _, col_a, col_b = group_info(g)
        return [
            pltpu.make_async_copy(whole.at[g, :, pl.ds(j * cols, cols)], out_hbm.at[:, pl.ds(col, cols)], out_sem.at[g, j])
            for j, col in enumerate((col_a, col_b))
        ]

    def stage0(g):
        slot, _, _ = group_info(g)
        start(resid_copies(g))

        @pl.when(g == 2)
        def _():
            x_wait_recv(4)
            xcopy(slot_ref(4), 12, right).start()
            xcopy(slot_ref(4), 6, sib).start()
            x_wait_recv(9)
            xcopy(slot_ref(9), 13, left).start()
            xcopy(slot_ref(9), 11, sib).start()

        @pl.when(g == 4)
        def _():
            x_wait_recv(5)
            xcopy(slot_ref(5), 7, sib).start()
            x_wait_recv(8)
            xcopy(slot_ref(8), 10, sib).start()

        @pl.when(g == 6)
        def _():
            x_wait_recv(12)
            xcopy(slot_ref(12), 14, sib).start()
            x_wait_recv(13)
            xcopy(slot_ref(13), 15, sib).start()

        for known, known_slot in enumerate((2, 3, 6, 11, 7, 10, 14, 15)):
            @pl.when(g == known)
            def _():
                x_wait_recv(known_slot)

        @pl.loop(0, act.shape[0] // 256)
        def _(m):
            where = pl.ds(pl.multiple_of(m * 256, 256), 256)
            value = jnp.dot(act[where, :], weight[lax.div(slot, 4) * 2 + lax.rem(slot, 2)], preferred_element_type=jnp.float32)
            part[pslot(g), where, :] = value.astype(jnp.bfloat16)

        for x in range(2):
            start(scatter_far(g, x, 1))

    def scatter_mid(level):
        def run(g):
            buf = recv1 if level == 1 else recv3
            rows = ROWS_L1 if level == 1 else ROWS_L2
            block = block1 if level == 1 else block2
            for x in range(2):
                finish(scatter_far(g, x, level))
                add_into(g, block(x, 1), rows // 2, buf[g, x, 0])
                add_into(g, offset(block(x, -1), rows // 2), rows // 2, buf[g, x, 1])
            for x in range(2):
                start(scatter_near(g, x, level))
        return run

    def stage2(g):
        for x in range(2):
            finish(scatter_near(g, x, 1))
            add_into(g, block1(x, 0), ROWS_L1, recv2[g, x, 0], recv2[g, x, 1])
        for x in range(2):
            start(scatter_far(g, x, 2))

    def stage4(g):
        finish(resid_copies(g))
        for x in range(2):
            finish(scatter_near(g, x, 2))
            whole[g, pl.ds(block2(x, 0), ROWS_L2), :] = summed(g, block2(x, 0), ROWS_L2, recv4[g, x, 0], recv4[g, x, 1], resid[g, x])
        for x in range(2):
            start(gather_near(g, x, 2))

    def relay(done, then):
        def run(g):
            for x in range(2):
                finish(done[0](g, x, done[1]))
                start(then[0](g, x, then[1]))
        return run

    def stage8(g):
        for x in range(2):
            finish(gather_far(g, x, 1))
        start(out_copies(g))

    stages = [
        stage0, scatter_mid(1), stage2, scatter_mid(2), stage4,
        relay((gather_near, 2), (gather_far, 2)), relay((gather_far, 2), (gather_near, 1)),
        relay((gather_near, 1), (gather_far, 1)), stage8,
    ]

    @pl.loop(0, (N_GROUPS // 2 - 1) * PERIOD + STAGES)
    def _(t):
        for s in reversed(range(STAGES)):
            d = t - s
            pair = lax.div(d + 4 * PERIOD, PERIOD) - 4
            starts = jnp.logical_and(lax.rem(d + 4 * PERIOD, PERIOD) == 0, jnp.logical_and(d >= 0, d < (N_GROUPS // 2) * PERIOD))

            @pl.when(starts)
            def _():
                stages[s](2 * pair)
                stages[s](2 * pair + 1)

    @pl.loop(0, N_GROUPS)
    def _(g):
        finish(out_copies(g))

    for slot, peer in own_sends:
        for copy in own_copies(slot, peer):
            copy.wait_send()
    for slot, peer in relays:
        xcopy(slot_ref(slot), slot, peer).wait_send()


def second_product(acts, pre, w_out, w_down, rows):
    seq_len = rows.shape[0]
    depth = w_out.shape[0] + w_down.shape[0]
    wide = w_out.shape[1]
    cols = wide // 2
    bf16 = jnp.bfloat16
    return pl.pallas_call(
        functools.partial(reduce_kernel, len(acts)),
        in_specs=[pl.BlockSpec(memory_space=pl.ANY)] * (len(acts) + 4),
        out_specs=pl.BlockSpec(memory_space=pl.ANY),
        out_shape=jax.ShapeDtypeStruct(rows.shape, bf16),
        scratch_shapes=[
            pltpu.VMEM((seq_len, depth), bf16),
            pltpu.VMEM((8, depth, wide), bf16),
            pltpu.VMEM((PART_SLOTS, seq_len, wide), bf16),
            pltpu.VMEM((N_GROUPS, seq_len, wide), bf16),
            pltpu.VMEM((N_GROUPS, 2, 2, ROWS_L1 // 2, wide), bf16),
            pltpu.VMEM((N_GROUPS, 2, 2, ROWS_L1, wide), bf16),
            pltpu.VMEM((N_GROUPS, 2, 2, ROWS_L2 // 2, wide), bf16),
            pltpu.VMEM((N_GROUPS, 2, 2, ROWS_L2, wide), bf16),
            pltpu.VMEM((N_GROUPS, 2, ROWS_L2, wide), bf16),
            pltpu.SemaphoreType.DMA((N_GROUPS, 2, 16)),
            pltpu.SemaphoreType.DMA((N_GROUPS, 2, 16)),
            pltpu.SemaphoreType.DMA((16, 2)),
            pltpu.SemaphoreType.DMA((16, 2)),
            pltpu.SemaphoreType.DMA((8 + len(acts),)),
            pltpu.SemaphoreType.DMA((N_GROUPS, 4)),
            pltpu.SemaphoreType.DMA((N_GROUPS, 2)),
        ],
        compiler_params=pltpu.CompilerParams(collective_id=0, has_side_effects=True, vmem_limit_bytes=62 * 1024 * 1024),
        cost_estimate=pl.CostEstimate(
            flops=2 * seq_len * depth * rows.shape[1], bytes_accessed=2 * (seq_len * depth + 8 * depth * wide + 2 * rows.size), transcendentals=0),
    )(*acts, pre, w_out, w_down, rows)


def solution(mesh):
    row_spec = P(("dp", "fsdp"), None, None)

    def local_layer(hidden, positions, norm_gain, w_query, w_key, w_value, w_gate, w_up, w_out, w_down):
        rows = hidden[0]
        cos_t, sin_t = rope_tables(positions, w_key.shape[1])
        *acts, pre = first_products(rows, norm_gain, w_query, w_key, w_value, w_gate, w_up, w_out, cos_t, sin_t)
        return second_product(acts, pre, w_out, w_down, rows)[None]

    in_specs = (row_spec, P(None), P("fsdp"), P("fsdp", "tp"), P("fsdp", None), P("fsdp", None), P("fsdp", "tp"), P("fsdp", "tp"), P("tp", "fsdp"), P("tp", "fsdp"))
    return jax.shard_map(local_layer, mesh=mesh, in_specs=in_specs, out_specs=row_spec, check_vma=False)
```

```python
import functools

import jax
import jax.numpy as jnp
import numpy as np
from jax import lax
from jax.experimental import pallas as pl
from jax.experimental.pallas import tpu as pltpu
from jax.sharding import PartitionSpec as P

MESH = pl.DeviceIdType.MESH
NORM_EPS = 1e-6


def rope_tables(positions, head_dim):
    inv_freq = 10000.0 ** (-jnp.arange(0, head_dim, 2, dtype=jnp.float32) / head_dim)
    angles = positions.astype(jnp.float32)[:, None] * inv_freq[None, :]
    angles = jnp.concatenate([angles, angles], axis=-1)
    return jnp.cos(angles), jnp.sin(angles)


FF_TILE = 256


def first_kernel(
    rows_hbm, gain_hbm, wq_hbm, wk_hbm, wv_hbm, wg_hbm, wu_hbm, wo_hbm, cos_ref, sin_ref, pick_ref, pick_rot_ref, place_ref,
    attn_hbm, z_hbm, pre_hbm,
    act, gains, wq, wk, wv, wff, q_heads, k_rot, values, zbuf,
    send_sem, recv_sem, gain_send, gain_recv, load_sem, act_sem, out_sem, pre_send, pre_recv,
):
    n = 8
    fs = lax.axis_index("fsdp")
    core = lax.rem(fs, 2)
    chip = lax.div(fs, 2)
    depth = wq_hbm.shape[0]
    half = depth // 2
    seq_len = rows_hbm.shape[0]
    n_chunks = wg_hbm.shape[1] // FF_TILE

    def device(by_chip, other):
        c = core if not other else 1 - core
        return lax.rem(chip + by_chip + 4, 4) * 2 + c

    right, left, sib = ({"fsdp": device(*p)} for p in ((1, 0), (-1, 0), (0, 1)))
    places = [(0, 0), (0, 1), (-1, 0), (-1, 1), (1, 0), (1, 1), (2, 0), (2, 1)]

    barrier = pltpu.get_barrier_semaphore()
    for by in range(1, n):
        pl.semaphore_signal(barrier, inc=1, device_id={"fsdp": lax.rem(fs + by, n)}, device_id_type=MESH)
    pl.semaphore_wait(barrier, n - 1)

    def qkv_streams():
        return [(0, wq_hbm, lambda at: wq.at[at, :]), (1, wk_hbm, lambda at: wk.at[:, at]), (2, wv_hbm, lambda at: wv.at[:, at])]

    def ff_streams(c):
        cols = pl.ds(pl.multiple_of(c * FF_TILE, FF_TILE), FF_TILE)
        return [
            (3 + 2 * c, wg_hbm.at[:, cols], lambda at: wff.at[c, at, pl.ds(0, FF_TILE)]),
            (4 + 2 * c, wu_hbm.at[:, cols], lambda at: wff.at[c, at, pl.ds(FF_TILE, FF_TILE)]),
        ]

    messages = [
        (2 * depth, depth, None, right), (4 * depth, depth, None, left),
        (6 * depth, half, 2 * depth, right), (6 * depth + half, half, 4 * depth + half, left),
        (depth, depth, None, sib), (3 * depth, depth, 2 * depth, sib), (5 * depth, depth, 4 * depth, sib),
        (7 * depth, half, 6 * depth, sib), (7 * depth + half, half, 6 * depth + half, sib),
    ]

    def message(stream, idx):
        row, own, gathered = stream
        dst, size, src, peer = messages[idx]
        return pltpu.make_async_remote_copy(
            src_ref=own if src is None else gathered(pl.ds(src, size)), dst_ref=gathered(pl.ds(dst, size)),
            send_sem=send_sem.at[row, idx], recv_sem=recv_sem.at[row, idx], device_id=peer, device_id_type=MESH)

    def own_load(stream):
        row, own, gathered = stream
        return pltpu.make_async_copy(own, gathered(pl.ds(0, depth)), load_sem.at[row])

    def send(streams, *idxs):
        for idx in idxs:
            for stream in streams:
                message(stream, idx).start()

    def receive(streams, *idxs):
        for idx in idxs:
            for stream in streams:
                message(stream, idx).wait_recv()

    def begin(streams):
        send(streams, 0, 1, 4)
        for stream in streams:
            own_load(stream).start()

    def pass_on(streams):
        receive(streams, 0, 1)
        send(streams, 2, 3, 5, 6)

    def complete(streams):
        receive(streams, 2, 3)
        send(streams, 7, 8)
        for stream in streams:
            own_load(stream).wait()
        receive(streams, 4, 5, 6, 7, 8)

    def gain_copy(slot):
        by_chip, other = places[slot]
        return pltpu.make_async_remote_copy(
            src_ref=gain_hbm, dst_ref=gains.at[pl.ds(slot * depth, depth)], send_sem=gain_send.at[slot], recv_sem=gain_recv.at[slot],
            device_id={"fsdp": device(-by_chip, other)}, device_id_type=MESH)

    for slot in range(1, n):
        gain_copy(slot).start()
    begin(qkv_streams())
    begin(ff_streams(0))
    own_gain = pltpu.make_async_copy(gain_hbm, gains.at[pl.ds(0, depth)], gain_send.at[0])
    own_gain.start()
    blocks = []
    for slot, place in enumerate(places):
        cols = pl.ds(pl.multiple_of(device(*place) * depth, 128), depth)
        blocks.append(pltpu.make_async_copy(rows_hbm.at[:, cols], act.at[:, pl.ds(slot * depth, depth)], act_sem.at[slot]))
    for block in blocks:
        block.start()
    own_gain.wait()
    for slot in range(1, n):
        gain_copy(slot).wait()
    for block in blocks:
        block.wait()

    @pl.loop(0, seq_len // 16)
    def _(r):
        where = pl.ds(pl.multiple_of(r * 16, 16), 16)
        row_f32 = act[where, :].astype(jnp.float32)
        centered = row_f32 - jnp.mean(row_f32, axis=-1, keepdims=True)
        variance = jnp.mean(centered * centered, axis=-1, keepdims=True)
        scaled = centered * lax.rsqrt(variance + NORM_EPS)
        for slot in range(n):
            cols = slice(slot * depth, (slot + 1) * depth)
            act[where, cols] = (scaled[:, cols] * gains[cols].reshape(1, depth)).astype(jnp.bfloat16)

    pass_on(qkv_streams())
    begin(ff_streams(1))
    pass_on(ff_streams(0))
    begin(ff_streams(2))
    complete(qkv_streams())

    n_heads, _, head_dim = pick_ref.shape

    def dot_t(a, b):
        return lax.dot_general(a, b, (((1,), (1,)), ((), ())), preferred_element_type=jnp.float32)

    q_block = 256

    @pl.loop(0, seq_len // q_block)
    def _(m):
        where = pl.ds(pl.multiple_of(m * q_block, q_block), q_block)
        cos_t, sin_t = cos_ref[where, :], sin_ref[where, :]
        dot = functools.partial(jnp.dot, preferred_element_type=jnp.float32)
        query_raw = dot(act[where, :], wq[...]).astype(jnp.bfloat16)
        for h in range(n_heads):
            rotated = dot(query_raw, pick_ref[h]) * cos_t + dot(query_raw, pick_rot_ref[h]) * sin_t
            q_heads[h, where, :] = rotated.astype(jnp.bfloat16)
        key_raw = dot_t(act[where, :], wk[...]).astype(jnp.bfloat16)
        key_turned = dot(key_raw, pick_rot_ref[0, 0:head_dim, :])
        k_rot[where, :] = (key_raw.astype(jnp.float32) * cos_t + key_turned * sin_t).astype(jnp.bfloat16)
        values[where, :] = dot_t(act[where, :], wv[...]).astype(jnp.bfloat16)

    for idx in range(9):
        message(qkv_streams()[0], idx).wait_send()
    pass_on(ff_streams(1))
    begin(ff_streams(3))

    score_scale = head_dim ** -0.5
    for blk in range(seq_len // q_block):
        lo, hi = blk * q_block, (blk + 1) * q_block
        causal_mask = lax.broadcasted_iota(jnp.int32, (q_block, hi), 1) <= lo + lax.broadcasted_iota(jnp.int32, (q_block, hi), 0)
        wq[lo:hi, :] = jnp.zeros((q_block, wq.shape[1]), jnp.bfloat16)

        @pl.loop(0, n_heads)
        def _(h):
            scores = dot_t(q_heads[h, lo:hi, :], k_rot[0:hi, :]) * score_scale
            scores = jnp.where(causal_mask, scores, -1e30)
            weights = jnp.exp(scores - jnp.max(scores, axis=-1, keepdims=True))
            prob_rows = (weights / jnp.sum(weights, axis=-1, keepdims=True)).astype(jnp.bfloat16)
            out = jnp.dot(prob_rows, values[0:hi, :], preferred_element_type=jnp.float32).astype(jnp.bfloat16)
            placed = jnp.dot(out, place_ref[h], preferred_element_type=jnp.float32).astype(jnp.bfloat16)
            wq[lo:hi, :] = wq[lo:hi, :] + placed

    attn_out = pltpu.make_async_copy(wq.at[pl.ds(0, seq_len), :], attn_hbm, out_sem.at[n_chunks])
    attn_out.start()

    def w_out_copy(side):
        return pltpu.make_async_remote_copy(
            src_ref=wo_hbm, dst_ref=pre_hbm.at[side], send_sem=pre_send.at[side], recv_sem=pre_recv.at[side],
            device_id=(right, left)[side], device_id_type=MESH)

    def z_out(c):
        cols = pl.ds(pl.multiple_of(c * FF_TILE, FF_TILE), FF_TILE)
        return pltpu.make_async_copy(zbuf.at[lax.rem(c, 2)], z_hbm.at[:, cols], out_sem.at[c])

    @pl.loop(0, n_chunks)
    def _(c):
        @pl.when(c + 2 < n_chunks)
        def _():
            pass_on(ff_streams(c + 2))

        @pl.when(c + 2 == n_chunks - 1)
        def _():
            for side in range(2):
                w_out_copy(side).start()

        @pl.when(c + 4 < n_chunks)
        def _():
            begin(ff_streams(c + 4))

        complete(ff_streams(c))

        @pl.when(c >= 2)
        def _():
            z_out(c - 2).wait()

        @pl.loop(0, seq_len // 256)
        def _(m):
            where = pl.ds(pl.multiple_of(m * 256, 256), 256)
            both = jnp.dot(act[where, :], wff[c], preferred_element_type=jnp.float32)
            gate = both[:, :FF_TILE].astype(jnp.bfloat16).astype(jnp.float32)
            up = both[:, FF_TILE:].astype(jnp.bfloat16).astype(jnp.float32)
            zbuf[lax.rem(c, 2), where, :] = (gate * jax.nn.sigmoid(gate) * up).astype(jnp.bfloat16)

        z_out(c).start()

    for c in (n_chunks - 2, n_chunks - 1):
        z_out(c).wait()
    attn_out.wait()
    for side in range(2):
        w_out_copy(side).wait()
    for stream in qkv_streams()[1:]:
        for idx in range(9):
            message(stream, idx).wait_send()

    @pl.loop(0, n_chunks)
    def _(c):
        for stream in ff_streams(c):
            for idx in range(9):
                message(stream, idx).wait_send()


def first_products(rows, norm_gain, w_query, w_key, w_value, w_gate, w_up, w_out, cos_t, sin_t):
    seq_len, width = rows.shape
    q_width, head_dim, ff = w_query.shape[1], w_key.shape[1], w_gate.shape[1]
    n_heads = q_width // head_dim
    n_chunks = ff // FF_TILE
    bf16 = jnp.bfloat16
    feature = np.arange(head_dim)
    head = np.arange(n_heads)[:, None, None] * head_dim
    source = np.arange(q_width)[None, :, None]
    one_hot = np.where(source == head + feature, 1.0, 0.0)
    turned = np.where(feature < head_dim // 2, feature + head_dim // 2, feature - head_dim // 2)
    sign = np.where(feature < head_dim // 2, -1.0, 1.0)
    pick = jnp.asarray(one_hot, bf16)
    pick_rot = jnp.asarray(np.where(source == head + turned, sign, 0.0), bf16)
    place = jnp.asarray(one_hot.transpose(0, 2, 1), bf16)
    hbm = pl.BlockSpec(memory_space=pl.ANY)
    vmem = pl.BlockSpec(memory_space=pltpu.VMEM)
    return pl.pallas_call(
        first_kernel,
        in_specs=[hbm] * 8 + [vmem] * 5,
        out_specs=[hbm] * 3,
        out_shape=[jax.ShapeDtypeStruct((seq_len, q_width), bf16), jax.ShapeDtypeStruct((seq_len, ff), bf16), jax.ShapeDtypeStruct((2, *w_out.shape), bf16)],
        scratch_shapes=[
            pltpu.VMEM((seq_len, width), bf16),
            pltpu.VMEM((width,), jnp.float32),
            pltpu.VMEM((width, q_width), bf16),
            pltpu.VMEM((head_dim, width), bf16),
            pltpu.VMEM((head_dim, width), bf16),
            pltpu.VMEM((n_chunks, width, 2 * FF_TILE), bf16),
            pltpu.VMEM((n_heads, seq_len, head_dim), bf16),
            pltpu.VMEM((seq_len, head_dim), bf16),
            pltpu.VMEM((seq_len, head_dim), bf16),
            pltpu.VMEM((2, seq_len, FF_TILE), bf16),
            pltpu.SemaphoreType.DMA((3 + 2 * n_chunks, 9)),
            pltpu.SemaphoreType.DMA((3 + 2 * n_chunks, 9)),
            pltpu.SemaphoreType.DMA((8,)),
            pltpu.SemaphoreType.DMA((8,)),
            pltpu.SemaphoreType.DMA((3 + 2 * n_chunks,)),
            pltpu.SemaphoreType.DMA((8,)),
            pltpu.SemaphoreType.DMA((n_chunks + 1,)),
            pltpu.SemaphoreType.DMA((2,)),
            pltpu.SemaphoreType.DMA((2,)),
        ],
        compiler_params=pltpu.CompilerParams(collective_id=1, has_side_effects=True, vmem_limit_bytes=67043328),
    )(rows, norm_gain, w_query, w_key.T, w_value.T, w_gate, w_up, w_out, cos_t, sin_t, pick, pick_rot, place)


ROWS_L1 = 128
ROWS_L2 = 32
N_GROUPS = 8
PERIOD = 3
STAGES = 9
SETTLE_PARTS = 16
PART_SLOTS = 6


def reduce_kernel(n_acts, *refs):
    acts_hbm = refs[:n_acts]
    reduce_body(acts_hbm, *refs[n_acts:])


def reduce_body(
    acts_hbm, pre_hbm, wo_hbm, wd_hbm, rows_hbm, out_hbm,
    act, weight, part, whole, recv1, recv2, recv3, recv4, resid,
    send_sem, recv_sem, xsend_sem, xrecv_sem, load_sem, resid_sem, out_sem,
):
    n_fsdp = 8
    tp = lax.axis_index("tp")
    fs = lax.axis_index("fsdp")
    coord = {"y": lax.rem(tp, 4), "z": lax.div(tp, 4)}
    core = lax.rem(fs, 2)
    full = wo_hbm.shape[1]
    cols = full // 2
    split = wo_hbm.shape[0]

    def at(axis, delta):
        moved = lax.rem(coord[axis] + delta + 4, 4)
        return {"tp": coord["z"] * 4 + moved if axis == "y" else moved * 4 + coord["y"]}

    right = {"fsdp": lax.rem(fs + 2, n_fsdp)}
    left = {"fsdp": lax.rem(fs + n_fsdp - 2, n_fsdp)}
    sib = {"fsdp": fs + 1 - 2 * core}

    def slot_ref(slot, rows=slice(None)):
        return weight.at[slot // 4 * 2 + slot % 2, rows, pl.ds(slot // 2 % 2 * cols, cols)]

    def xcopy(src, slot, peer):
        return pltpu.make_async_remote_copy(
            src_ref=src, dst_ref=slot_ref(slot), send_sem=xsend_sem.at[slot, 0], recv_sem=xrecv_sem.at[slot, 0],
            device_id=peer, device_id_type=MESH)

    def own_parts(half):
        where = pl.ds(half * cols, cols)
        return [(wo_hbm.at[:, where], pl.ds(0, split)), (wd_hbm.at[:, where], pl.ds(split, wd_hbm.shape[0]))]

    def own_copies(slot, peer):
        return [
            pltpu.make_async_remote_copy(
                src_ref=src, dst_ref=slot_ref(slot, into), send_sem=xsend_sem.at[slot, j], recv_sem=xrecv_sem.at[slot, j],
                device_id=peer, device_id_type=MESH)
            for j, (src, into) in enumerate(own_parts(slot % 2)) if j or slot in (2, 3)
        ]

    own_sends = [(4, right), (9, left), (2, sib), (5, right), (8, left), (3, sib)]
    relays = [(6, sib), (7, sib), (10, sib), (11, sib), (12, right), (13, left), (14, sib), (15, sib)]

    def x_wait_recv(slot):
        if slot in (2, 3, 4, 5, 8, 9):
            for copy in own_copies(slot, sib):
                copy.wait_recv()
        else:
            xcopy(slot_ref(slot), slot, sib).wait_recv()

    def own_loads(half):
        return [
            pltpu.make_async_copy(src, slot_ref(half, part_rows), load_sem.at[2 * half + j])
            for j, (src, part_rows) in enumerate(own_parts(half))
        ]

    def early_loads():
        return [
            pltpu.make_async_copy(
                pre_hbm.at[side, :, pl.ds(half * cols, cols)], slot_ref(4 + 4 * side + half, pl.ds(0, split)), load_sem.at[4 + 2 * side + half])
            for side in range(2) for half in range(2)
        ]

    act_loads = []
    col = 0
    for idx, act_hbm in enumerate(acts_hbm):
        size = act_hbm.shape[1]
        act_loads.append(pltpu.make_async_copy(act_hbm, act.at[:, pl.ds(col, size)], load_sem.at[8 + idx]))
        col += size
    for load in act_loads + own_loads(0) + own_loads(1) + early_loads():
        load.start()

    barrier = pltpu.get_barrier_semaphore()
    peers = [at("y", 1), at("y", -1), at("z", 1), at("z", -1), right, left, sib]
    for peer in peers:
        pl.semaphore_signal(barrier, inc=1, device_id=peer, device_id_type=MESH)
    pl.semaphore_wait(barrier, len(peers))

    for slot, peer in own_sends:
        for copy in own_copies(slot, peer):
            copy.start()
    for load in act_loads + own_loads(0):
        load.wait()

    halves = [("y", "z"), ("z", "y")]

    def pslot(g):
        return lax.rem(g, PART_SLOTS)

    def block1(x, delta):
        k = lax.rem(coord[halves[x][0]] + delta + 4, 4)
        return pl.multiple_of(x * 4 * ROWS_L1 + k * ROWS_L1, ROWS_L1)

    def block2(x, delta):
        k = lax.rem(coord[halves[x][1]] + delta + 4, 4)
        return pl.multiple_of(block1(x, 0) + k * ROWS_L2, ROWS_L2)

    def offset(base, add):
        return pl.multiple_of(base + add, 16)

    def message(g, x, kind, src, dst, axis, delta):
        return pltpu.make_async_remote_copy(
            src_ref=src, dst_ref=dst, send_sem=send_sem.at[g, x, kind], recv_sem=recv_sem.at[g, x, kind],
            device_id=at(axis, delta), device_id_type=MESH)

    def scatter_far(g, x, level):
        block, axis, buf, rows, kind = (block1, halves[x][0], recv1, ROWS_L1, 0) if level == 1 else (block2, halves[x][1], recv3, ROWS_L2, 4)
        half = rows // 2
        far = block(x, 2)
        return [
            message(g, x, kind, part.at[pslot(g), pl.ds(far, half), :], buf.at[g, x, 0], axis, 1),
            message(g, x, kind + 1, part.at[pslot(g), pl.ds(offset(far, half), half), :], buf.at[g, x, 1], axis, -1),
        ]

    def scatter_near(g, x, level):
        block, axis, buf, rows, kind = (block1, halves[x][0], recv2, ROWS_L1, 2) if level == 1 else (block2, halves[x][1], recv4, ROWS_L2, 6)
        return [
            message(g, x, kind, part.at[pslot(g), pl.ds(block(x, 1), rows), :], buf.at[g, x, 0], axis, 1),
            message(g, x, kind + 1, part.at[pslot(g), pl.ds(block(x, -1), rows), :], buf.at[g, x, 1], axis, -1),
        ]

    def gather_near(g, x, level):
        block, axis, rows, kind = (block1, halves[x][0], ROWS_L1, 12) if level == 1 else (block2, halves[x][1], ROWS_L2, 8)
        mine = whole.at[g, pl.ds(block(x, 0), rows), :]
        return [message(g, x, kind, mine, mine, axis, 1), message(g, x, kind + 1, mine, mine, axis, -1)]

    def gather_far(g, x, level):
        block, axis, rows, kind = (block1, halves[x][0], ROWS_L1, 14) if level == 1 else (block2, halves[x][1], ROWS_L2, 10)
        half = rows // 2
        lo = whole.at[g, pl.ds(block(x, -1), half), :]
        hi = whole.at[g, pl.ds(offset(block(x, 1), half), half), :]
        return [message(g, x, kind, lo, lo, axis, 1), message(g, x, kind + 1, hi, hi, axis, -1)]

    def start(copies):
        for copy in copies:
            copy.start()

    def finish(copies):
        for copy in copies:
            copy.wait()

    def summed(g, row, rows, *refs):
        total = part[pslot(g), pl.ds(row, rows), :].astype(jnp.float32)
        for ref in refs:
            total = total + ref.astype(jnp.float32)
        return total.astype(jnp.bfloat16)

    def add_into(g, row, rows, *refs):
        part[pslot(g), pl.ds(row, rows), :] = summed(g, row, rows, *refs)

    def group_info(g):
        mid = jnp.logical_and(g >= 2, g < 6)
        second, late = lax.rem(g, 2), lax.div(g, 4)
        half = jnp.where(mid, lax.rem(second + late, 2), second)
        slot = jnp.where(g < 2, g, jnp.where(mid, 4 + 4 * second + half, g + 6))
        delta = jnp.where(g < 2, 0, jnp.where(mid, 2 * second - 1, 2))
        chip = lax.rem(lax.div(fs, 2) + delta + 4, 4)
        col_a = pl.multiple_of((chip * 2 + core) * full + half * cols, 128)
        col_b = pl.multiple_of((chip * 2 + 1 - core) * full + half * cols, 128)
        return slot, col_a, col_b

    def resid_copies(g):
        _, col_a, col_b = group_info(g)
        copies = []
        for x in range(2):
            for j, col in enumerate((col_a, col_b)):
                copies.append(pltpu.make_async_copy(
                    rows_hbm.at[pl.ds(block2(x, 0), ROWS_L2), pl.ds(col, cols)],
                    resid.at[g, x, :, pl.ds(j * cols, cols)], resid_sem.at[g, 2 * x + j]))
        return copies

    def out_copies(g):
        _, col_a, col_b = group_info(g)
        return [
            pltpu.make_async_copy(whole.at[g, :, pl.ds(j * cols, cols)], out_hbm.at[:, pl.ds(col, cols)], out_sem.at[g, j])
            for j, col in enumerate((col_a, col_b))
        ]

    def stage0(g):
        slot, _, _ = group_info(g)
        start(resid_copies(g))

        @pl.when(g == 1)
        def _():
            for load in own_loads(1):
                load.wait()

        @pl.when(g == 2)
        def _():
            for load in early_loads():
                load.wait()
            x_wait_recv(4)
            xcopy(slot_ref(4), 12, right).start()
            xcopy(slot_ref(4), 6, sib).start()
            x_wait_recv(9)
            xcopy(slot_ref(9), 13, left).start()
            xcopy(slot_ref(9), 11, sib).start()

        @pl.when(g == 4)
        def _():
            x_wait_recv(5)
            xcopy(slot_ref(5), 7, sib).start()
            x_wait_recv(8)
            xcopy(slot_ref(8), 10, sib).start()

        @pl.when(g == 6)
        def _():
            x_wait_recv(12)
            xcopy(slot_ref(12), 14, sib).start()
            x_wait_recv(13)
            xcopy(slot_ref(13), 15, sib).start()

        for known, known_slot in enumerate((2, 3, 6, 11, 7, 10, 14, 15)):
            @pl.when(g == known)
            def _():
                x_wait_recv(known_slot)

        columns = weight.at[lax.div(slot, 4) * 2 + lax.rem(slot, 2)]

        def product(delta):
            where = [pl.ds(block1(x, delta), ROWS_L1) for x in range(2)]
            both = jnp.concatenate([act[rows, :] for rows in where], axis=0)
            value = jnp.dot(both, columns[...], preferred_element_type=jnp.float32).astype(jnp.bfloat16)
            for x, rows in enumerate(where):
                part[pslot(g), rows, :] = value[x * ROWS_L1 : (x + 1) * ROWS_L1]

        product(2)
        for x in range(2):
            start(scatter_far(g, x, 1))

        @pl.loop(0, 3)
        def _(k):
            product(k - 1)

    def scatter_mid(level):
        def run(g):
            buf = recv1 if level == 1 else recv3
            rows = ROWS_L1 if level == 1 else ROWS_L2
            block = block1 if level == 1 else block2
            for x in range(2):
                finish(scatter_far(g, x, level))
                add_into(g, block(x, 1), rows // 2, buf[g, x, 0])
                add_into(g, offset(block(x, -1), rows // 2), rows // 2, buf[g, x, 1])
            for x in range(2):
                start(scatter_near(g, x, level))
        return run

    def stage2(g):
        for x in range(2):
            finish(scatter_near(g, x, 1))
            add_into(g, block1(x, 0), ROWS_L1, recv2[g, x, 0], recv2[g, x, 1])
        for x in range(2):
            start(scatter_far(g, x, 2))

    def stage4(g):
        finish(resid_copies(g))
        for x in range(2):
            finish(scatter_near(g, x, 2))
            whole[g, pl.ds(block2(x, 0), ROWS_L2), :] = summed(g, block2(x, 0), ROWS_L2, recv4[g, x, 0], recv4[g, x, 1], resid[g, x])
        for x in range(2):
            start(gather_near(g, x, 2))

    def relay(done, then):
        def run(g):
            for x in range(2):
                finish(done[0](g, x, done[1]))
                start(then[0](g, x, then[1]))
        return run

    def stage8(g):
        for x in range(2):
            finish(gather_far(g, x, 1))
        start(out_copies(g))

    stages = [
        stage0, scatter_mid(1), stage2, scatter_mid(2), stage4,
        relay((gather_near, 2), (gather_far, 2)), relay((gather_far, 2), (gather_near, 1)),
        relay((gather_near, 1), (gather_far, 1)), stage8,
    ]

    @pl.loop(0, (N_GROUPS // 2 - 1) * PERIOD + STAGES)
    def _(t):
        for s in reversed(range(STAGES)):
            d = t - s
            pair = lax.div(d + 4 * PERIOD, PERIOD) - 4
            starts = jnp.logical_and(lax.rem(d + 4 * PERIOD, PERIOD) == 0, jnp.logical_and(d >= 0, d < (N_GROUPS // 2) * PERIOD))

            @pl.when(starts)
            def _():
                stages[s](2 * pair)
                stages[s](2 * pair + 1)

    @pl.loop(0, N_GROUPS)
    def _(g):
        finish(out_copies(g))

    for slot, peer in own_sends:
        for copy in own_copies(slot, peer):
            copy.wait_send()
    for slot, peer in relays:
        xcopy(slot_ref(slot), slot, peer).wait_send()


def second_product(acts, pre, w_out, w_down, rows):
    seq_len = rows.shape[0]
    depth = w_out.shape[0] + w_down.shape[0]
    wide = w_out.shape[1]
    cols = wide // 2
    bf16 = jnp.bfloat16
    return pl.pallas_call(
        functools.partial(reduce_kernel, len(acts)),
        in_specs=[pl.BlockSpec(memory_space=pl.ANY)] * (len(acts) + 4),
        out_specs=pl.BlockSpec(memory_space=pl.ANY),
        out_shape=jax.ShapeDtypeStruct(rows.shape, bf16),
        scratch_shapes=[
            pltpu.VMEM((seq_len, depth), bf16),
            pltpu.VMEM((8, depth, wide), bf16),
            pltpu.VMEM((PART_SLOTS, seq_len, wide), bf16),
            pltpu.VMEM((N_GROUPS, seq_len, wide), bf16),
            pltpu.VMEM((N_GROUPS, 2, 2, ROWS_L1 // 2, wide), bf16),
            pltpu.VMEM((N_GROUPS, 2, 2, ROWS_L1, wide), bf16),
            pltpu.VMEM((N_GROUPS, 2, 2, ROWS_L2 // 2, wide), bf16),
            pltpu.VMEM((N_GROUPS, 2, 2, ROWS_L2, wide), bf16),
            pltpu.VMEM((N_GROUPS, 2, ROWS_L2, wide), bf16),
            pltpu.SemaphoreType.DMA((N_GROUPS, 2, 16)),
            pltpu.SemaphoreType.DMA((N_GROUPS, 2, 16)),
            pltpu.SemaphoreType.DMA((16, 2)),
            pltpu.SemaphoreType.DMA((16, 2)),
            pltpu.SemaphoreType.DMA((8 + len(acts),)),
            pltpu.SemaphoreType.DMA((N_GROUPS, 4)),
            pltpu.SemaphoreType.DMA((N_GROUPS, 2)),
        ],
        compiler_params=pltpu.CompilerParams(collective_id=0, has_side_effects=True, vmem_limit_bytes=62 * 1024 * 1024),
        cost_estimate=pl.CostEstimate(
            flops=2 * seq_len * depth * rows.shape[1], bytes_accessed=2 * (seq_len * depth + 8 * depth * wide + 2 * rows.size), transcendentals=0),
    )(*acts, pre, w_out, w_down, rows)


def settle_kernel(src_hbm, out_hbm, buffer, in_sem, out_sem):
    loads = [pltpu.make_async_copy(src_hbm.at[rows], buffer.at[rows], in_sem.at[k]) for k, rows in enumerate(settle_rows(src_hbm))]
    stores = [pltpu.make_async_copy(buffer.at[rows], out_hbm.at[rows], out_sem.at[k]) for k, rows in enumerate(settle_rows(src_hbm))]
    for load in loads:
        load.start()
    for load, store in zip(loads, stores):
        load.wait()
        store.start()
    for store in stores:
        store.wait()


def settle_rows(ref):
    size = ref.shape[0] // SETTLE_PARTS
    return [pl.ds(k * size, size) for k in range(SETTLE_PARTS)]


def settle(result):
    return pl.pallas_call(
        settle_kernel,
        in_specs=[pl.BlockSpec(memory_space=pl.ANY)],
        out_specs=pl.BlockSpec(memory_space=pl.ANY),
        out_shape=jax.ShapeDtypeStruct(result.shape, result.dtype),
        scratch_shapes=[
            pltpu.VMEM(result.shape, result.dtype),
            pltpu.SemaphoreType.DMA((SETTLE_PARTS,)),
            pltpu.SemaphoreType.DMA((SETTLE_PARTS,)),
        ],
        compiler_params=pltpu.CompilerParams(vmem_limit_bytes=62 * 1024 * 1024),
    )(result)


def solution(mesh):
    row_spec = P(("dp", "fsdp"), None, None)

    def local_layer(hidden, positions, norm_gain, w_query, w_key, w_value, w_gate, w_up, w_out, w_down):
        rows = hidden[0]
        cos_t, sin_t = rope_tables(positions, w_key.shape[1])
        *acts, pre = first_products(rows, norm_gain, w_query, w_key, w_value, w_gate, w_up, w_out, cos_t, sin_t)
        return settle(second_product(acts, pre, w_out, w_down, rows))[None]

    in_specs = (row_spec, P(None), P("fsdp"), P("fsdp", "tp"), P("fsdp", None), P("fsdp", None), P("fsdp", "tp"), P("fsdp", "tp"), P("tp", "fsdp"), P("tp", "fsdp"))
    return jax.shard_map(local_layer, mesh=mesh, in_specs=in_specs, out_specs=row_spec, check_vma=False)
```
